128 devices in a mesh: rows: 16 (over x, y), cols: 8 (over z, core).
Axes of the slice: x: 4, y: 4, z: 4, core: 2. Of those that a mesh axis runs over, the one named last changes fastest.
Arguments:
- coarse: float32 [1024, 1024], P('rows', 'cols'), may hold values from -6 to 6
- detail4: float32 [3, 1024, 1024], P(None, 'rows', 'cols'), may hold values from -6 to 6
- detail3: float32 [3, 2048, 2048], P(None, 'rows', 'cols'), may hold values from -6 to 6
- detail2: float32 [3, 4096, 4096], P(None, 'rows', 'cols'), may hold values from -6 to 6
- detail1: float32 [3, 8192, 8192], P(None, 'rows', 'cols'), may hold values from -6 to 6
Outputs:
- image: float32 [16384, 16384], P('rows', 'cols')
The draws below stay inside these ranges and needn't reach their ends.
All inputs are finite; a program needn't handle non-finite values.
Results may differ from the reference program's by a relative error of at most 0.00013.
Values sent between devices are 32-bit elements; how exact they have to be, the bound alone decides.
No kernel may reach another device: no remote copies, remote signals or barrier semaphores. Data moves between devices by JAX's collectives and lax.ppermute only.
A program may use at most 128 MiB of HBM per device.

```python
import jax
import jax.numpy as jnp

NR = 16384
NC = 16384


def steps_of(rng, dims, shards, smallest, high):
    def one(position, blocks):
        draws = jax.random.uniform(jax.random.fold_in(jax.random.fold_in(rng, 6), position), (blocks,), jnp.float32, smallest / len(shards), high / len(shards))
        return jnp.repeat(jnp.exp(draws), dims[position] // blocks).reshape((-1,) + (1,) * (len(dims) - position - 1))

    loudness = one(*shards[0])
    for cut in shards[1:]:
        loudness = loudness * one(*cut)
    return loudness


def noise(own_key, extent, deviation, reach, cuts=(), kind=jnp.bfloat16):
    result = deviation * jax.random.normal(own_key, extent, jnp.float32)
    if cuts:
        result = result * steps_of(own_key, extent, cuts, -0.22, 0.18)
    return jnp.clip(result, -reach, reach).astype(kind)


def setup_inputs(seed: int = 0) -> dict:
    splits = jax.random.split(jax.random.key(seed), 6)
    coarse = noise(splits[0], (NR // 16, NC // 16), 1.0, 6.0, ((0, 16), (1, 8)), jnp.float32)
    detail4 = noise(splits[1], (3, NR // 16, NC // 16), 1.0, 6.0, ((1, 16), (2, 8)), jnp.float32)
    detail3 = noise(splits[2], (3, NR // 8, NC // 8), 1.0, 6.0, ((1, 16), (2, 8)), jnp.float32)
    detail2 = noise(splits[3], (3, NR // 4, NC // 4), 1.0, 6.0, ((1, 16), (2, 8)), jnp.float32)
    detail1 = noise(splits[4], (3, NR // 2, NC // 2), 1.0, 6.0, ((1, 16), (2, 8)), jnp.float32)
    return {"coarse": coarse, "detail4": detail4, "detail3": detail3, "detail2": detail2, "detail1": detail1}


lift_alpha = -1.586134342059924
lift_beta = -0.052980118572961
lift_gamma = 0.882911075530934
lift_delta = 0.443506852043971
lift_scale = 1.149604398860241


def phase_join(smooth, rough, along):
    target = list(smooth.shape)
    target[along] = 2 * target[along]
    return jnp.stack((smooth, rough), axis=along + 1).reshape(target)


def lift_roll(smooth, rough, along):
    smooth = smooth * lift_scale
    rough = rough / lift_scale
    smooth = smooth - lift_delta * (rough + jnp.roll(rough, 1, along))
    rough = rough - lift_gamma * (smooth + jnp.roll(smooth, -1, along))
    smooth = smooth - lift_beta * (rough + jnp.roll(rough, 1, along))
    rough = rough - lift_alpha * (smooth + jnp.roll(smooth, -1, along))
    return phase_join(smooth, rough, along)


def whole_synth(lowband, detail):
    smooth = jnp.stack((lowband, detail[1]), 0)
    rough = jnp.stack((detail[0], detail[2]), 0)
    halves = lift_roll(smooth, rough, 2)
    return lift_roll(halves[0], halves[1], 0)


def reference(coarse, detail4, detail3, detail2, detail1):
    lowband = coarse
    for detail in (detail4, detail3, detail2, detail1):
        lowband = whole_synth(lowband, detail)
    return lowband
```

```python
import functools

import jax
import jax.numpy as jnp
from jax import lax
from jax.experimental import pallas as pl
from jax.experimental.pallas import tpu as pltpu
from jax.sharding import PartitionSpec as P

lift_alpha = -1.586134342059924
lift_beta = -0.052980118572961
lift_gamma = 0.882911075530934
lift_delta = 0.443506852043971
lift_scale = 1.149604398860241
SQ = lift_scale * lift_scale

H = (512, 256, 128, 64)
W = (1024, 512, 256, 128)
PLANES = tuple((k, p) for k in range(4) for p in range(3)) + ((3, 3),)
ROFF = []
COFF = []
_r = _c = 0
for _k, _p in PLANES:
    ROFF.append(_r)
    COFF.append(_c)
    _r += W[_k]
    _c += H[_k] // 8 + 1
RW = _r
CG = _c
HALF = RW // 2
PK = -(-CG // 32)

f32 = jnp.float32
bf16 = jnp.bfloat16


def iota(shape, dim):
    return lax.broadcasted_iota(jnp.int32, shape, dim)


def row_pack_kernel(*refs):
    tops, bots = refs[0:5], refs[5:10]
    up, down = refs[10], refs[11]
    top, bot = [], []
    for k, p in PLANES:
        if p == 3:
            top.append(tops[4][...])
            bot.append(bots[4][...])
        else:
            top.append(tops[k][p])
            bot.append(bots[k][p])
    top = jnp.concatenate(top, axis=1)
    bot = jnp.concatenate(bot, axis=1)
    low = iota((8, HALF), 0) < 4
    up[...] = jnp.where(low, top[:, :HALF], pltpu.roll(top[:, HALF:], 4, 0))
    down[...] = jnp.where(low, pltpu.roll(bot[:, :HALF], 4, 0), bot[:, HALF:])


def row_pack(coarse, details):
    def spec(k, last):
        row = H[k] // 8 - 1 if last else 0
        return pl.BlockSpec((3, 8, W[k]), lambda i: (0, row, 0))

    def cspec(last):
        row = H[3] // 8 - 1 if last else 0
        return pl.BlockSpec((8, W[3]), lambda i: (row, 0))

    specs = [spec(k, False) for k in range(4)] + [cspec(False)]
    specs += [spec(k, True) for k in range(4)] + [cspec(True)]
    out = jax.ShapeDtypeStruct((8, HALF), f32)
    return pl.pallas_call(
        row_pack_kernel,
        grid=(1,),
        in_specs=specs,
        out_specs=[pl.BlockSpec((8, HALF), lambda i: (0, 0))] * 2,
        out_shape=[out, out],
        name="row_pack",
    )(*details, coarse, *details, coarse)


def row_unpack(after, before):
    low = iota(after.shape, 0) < 4
    first = jnp.where(low, after, pltpu.roll(before, 4, 0))
    second = jnp.where(low, pltpu.roll(after, 4, 0), before)
    return first, second


def col_pack_kernel(*refs):
    lefts, rights = refs[0:5], refs[5:10]
    after, before = refs[10], refs[11]
    left_out, right_out = refs[12], refs[13]
    first, second = row_unpack(after[...], before[...])
    ext = jnp.concatenate([first, second], axis=1)
    lane = iota((8, 128), 1)

    def edge(q):
        n = max(i for i in range(13) if COFF[i] <= q)
        k, p = PLANES[n]
        g = q - COFF[n]
        if g == H[k] // 8:
            o = ROFF[n]
            lo, hi = ext[:, o : o + 128], ext[:, o + W[k] - 128 : o + W[k]]
        elif p == 3:
            lo, hi = lefts[4][8 * g : 8 * g + 8, :], rights[4][8 * g : 8 * g + 8, :]
        else:
            lo, hi = lefts[k][p, 8 * g : 8 * g + 8, :], rights[k][p, 8 * g : 8 * g + 8, :]
        return jnp.where(lane < 64, lo, hi)

    lacc = [jnp.zeros((8, 128), f32) for _ in range(PK)]
    racc = [jnp.zeros((8, 128), f32) for _ in range(PK)]
    for j in range(32):
        start = 4 * j
        nxt = (4 * j + 4) % 128
        rmask = (lane >= start) & (lane < start + 4)
        lmask = (lane >= nxt) & (lane < nxt + 4)
        for m in range(PK):
            q = 32 * m + j
            if q < CG:
                e = edge(q)
                if nxt:
                    e = pltpu.roll(e, nxt, 1)
                lacc[m] = jnp.where(lmask, e, lacc[m])
                racc[m] = jnp.where(rmask, e, racc[m])
    for m in range(PK):
        left_out[8 * m : 8 * m + 8, :] = lacc[m]
        right_out[8 * m : 8 * m + 8, :] = racc[m]


def col_pack(coarse, details, after, before):
    def spec(k, last):
        col = W[k] // 128 - 1 if last else 0
        return pl.BlockSpec((3, H[k], 128), lambda i: (0, 0, col))

    def cspec(last):
        col = W[3] // 128 - 1 if last else 0
        return pl.BlockSpec((H[3], 128), lambda i: (0, col))

    specs = [spec(k, False) for k in range(4)] + [cspec(False)]
    specs += [spec(k, True) for k in range(4)] + [cspec(True)]
    specs += [pl.BlockSpec((8, HALF), lambda i: (0, 0))] * 2
    out = jax.ShapeDtypeStruct((8 * PK, 128), f32)
    return pl.pallas_call(
        col_pack_kernel,
        grid=(1,),
        in_specs=specs,
        out_specs=[pl.BlockSpec((8 * PK, 128), lambda i: (0, 0))] * 2,
        out_shape=[out, out],
        name="col_pack",
    )(*details, coarse, *details, coarse, after, before)


def vertical(load_s, load_r, groups, store_s, store_r):
    sub = iota((8, 128), 0)
    first, last = sub == 0, sub == 7
    memo = {}

    def cached(f):
        def get(g):
            g = g % groups
            if (f, g) not in memo:
                memo[(f, g)] = f(g)
            return memo[(f, g)]

        return get

    s = cached(lambda g: load_s(g))
    r = cached(lambda g: load_r(g))

    def prev_of(x):
        turned = cached(lambda g: pltpu.roll(x(g), 1, 0))
        return lambda g: jnp.where(first, turned(g - 1), turned(g))

    def next_of(x):
        turned = cached(lambda g: pltpu.roll(x(g), 7, 0))
        return lambda g: jnp.where(last, turned(g + 1), turned(g))

    rp = prev_of(r)
    s1 = cached(lambda g: s(g) - lift_delta * (r(g) + rp(g)))
    s1n = next_of(s1)
    r1 = cached(lambda g: r(g) - lift_gamma * (s1(g) + s1n(g)))
    r1p = prev_of(r1)
    s2 = cached(lambda g: s1(g) - lift_beta * (r1(g) + r1p(g)))
    s2n = next_of(s2)
    r2 = cached(lambda g: r1(g) - lift_alpha * (s2(g) + s2n(g)))
    for g in range(groups):
        store_s(g, s2(g))
        store_r(g, r2(g))


def horizontal(s, r):
    n = s.shape[1]
    s = s - lift_delta * (r + pltpu.roll(r, 1, 1))
    r = r - lift_gamma * (s + pltpu.roll(s, n - 1, 1))
    s = s - lift_beta * (r + pltpu.roll(r, 1, 1))
    r = r - lift_alpha * (s + pltpu.roll(s, n - 1, 1))
    return s, r


def interleave(s, r, blocks, perm):
    rows = s.shape[0]
    x = jnp.concatenate(
        [
            jnp.concatenate([s[:, 128 * b : 128 * b + 128], r[:, 128 * b : 128 * b + 128]], axis=1)
            for b in range(blocks)
        ],
        axis=0,
    )
    hi = x.astype(bf16)
    lo = (x - hi.astype(f32)).astype(bf16)
    y = jnp.dot(jnp.concatenate([hi, lo], axis=1), perm, preferred_element_type=f32)
    return [y[rows * b : rows * b + rows, :] for b in range(blocks)]


ROWS = 64
SLOTS = 4


def main_kernel(
    coarse, d4, d3, d2, d1, rafter, rbefore, cafter, cbefore, out,
    xr, xc, u, v, l3, l2, l1, perm, stage, sems,
):
    details = (d1, d2, d3, d4)
    lows = (l1, l2, l3)
    lane = iota((8, 128), 1)
    first, second = row_unpack(rafter[...], rbefore[...])
    xr[:, :HALF] = first
    xr[:, HALF:] = second

    even = (iota((8 * PK, 128), 1) % 8) < 4
    aft, bef = cafter[...], cbefore[...]
    comb = (jnp.where(even, bef, aft), jnp.where(even, aft, bef))
    keep = (lane < 4) | (lane >= 124)
    for q in range(CG):
        m, j = divmod(q, 32)
        t = comb[j % 2][8 * m : 8 * m + 8, :]
        shift = (124 - 4 * j) % 128
        if shift:
            t = pltpu.roll(t, shift, 1)
        xc[8 * q : 8 * q + 8, :] = jnp.where(keep, t, 0.0)

    row = iota((512, 256), 0) % 256
    col = iota((512, 256), 1)
    target = jnp.where(row < 128, 2 * row, 2 * row - 255)
    perm[...] = jnp.where(col == target, 1.0, 0.0).astype(bf16)

    for k in (3, 2, 1, 0):
        h, w = H[k], W[k]
        groups, blocks = h // 8 + 1, w // 128

        def load(p, g, b, k=k, h=h, w=w, groups=groups, blocks=blocks):
            static = isinstance(b, int)
            n = 3 * k + p if p < 3 else 12
            if p == 3 and k < 3:
                at = 128 * b if static else pl.multiple_of(b * 128, 128)
                return lows[k][8 * g : 8 * g + 8, pl.ds(at, 128)]
            if static and b == blocks:
                q = COFF[n] + g
                return xc[8 * q : 8 * q + 8, :]
            if g == groups - 1:
                at = ROFF[n] + 128 * b
                if not static:
                    at = pl.multiple_of(at, 128)
                return xr[:, pl.ds(at, 128)]
            at = 128 * b if static else pl.multiple_of(b * 128, 128)
            if p == 3:
                return coarse[8 * g : 8 * g + 8, pl.ds(at, 128)]
            return details[k][p, 8 * g : 8 * g + 8, pl.ds(at, 128)]

        def columns(b, load=load, groups=groups, k=k):
            def store(ref, odd):
                def put(g, x):
                    if k == 0 and g == groups - 1:
                        return
                    ref[b, pl.ds(16 * g + odd, 8, 2), :] = x

                return put

            vertical(
                lambda g: load(3, g, b) * SQ, lambda g: load(1, g, b), groups, store(u, 0), store(u, 1)
            )
            vertical(
                lambda g: load(0, g, b), lambda g: load(2, g, b) * (1.0 / SQ), groups, store(v, 0), store(v, 1)
            )

        if blocks > 1:
            def body(b, c, columns=columns):
                columns(b)
                return c

            lax.fori_loop(0, blocks, body, 0)
        else:
            columns(0)
        columns(blocks)

        def rows_of(at, rows, blocks=blocks):
            s = jnp.concatenate([u[b, pl.ds(at, rows), :] for b in range(blocks + 1)], axis=1)
            r = jnp.concatenate([v[b, pl.ds(at, rows), :] for b in range(blocks + 1)], axis=1)
            return horizontal(s, r)

        if k:
            low = lows[k - 1]
            total = 16 * groups
            rows = {3: 144, 2: 136, 1: 88}[k]

            def chunk(i, c, rows=rows, rows_of=rows_of, low=low, blocks=blocks):
                at = pl.multiple_of(i * rows, 8)
                s, r = rows_of(at, rows)
                parts = interleave(s, r, blocks + 1, perm[...])
                for b in range(blocks):
                    low[pl.ds(at, rows), 256 * b : 256 * b + 256] = parts[b]
                left, right = parts[blocks][:, :128], parts[blocks][:, 128:]
                low[pl.ds(at, rows), 256 * blocks : 256 * blocks + 128] = jnp.where(
                    iota((rows, 128), 1) < 64, left, right
                )
                return c

            lax.fori_loop(0, total // rows, chunk, 0)
            top = low[2 * h : 2 * h + 8, :]
            bottom = low[2 * h + 8 : 2 * h + 16, :]
            low[2 * h : 2 * h + 8, :] = jnp.where(iota(top.shape, 0) < 4, top, bottom)
        else:
            def copy(i, slot):
                return pltpu.make_async_copy(
                    stage.at[slot], out.at[pl.ds(pl.multiple_of(i * ROWS, 8), ROWS), :], sems.at[slot]
                )

            def chunk(i, c, rows_of=rows_of, blocks=blocks):
                slot = lax.rem(i, SLOTS)

                @pl.when(i >= SLOTS)
                def _():
                    copy(i - SLOTS, slot).wait()

                s, r = rows_of(pl.multiple_of(i * ROWS, 8), ROWS)
                parts = interleave(s, r, blocks, perm[...])
                for b in range(blocks):
                    stage[slot, :, 256 * b : 256 * b + 256] = parts[b]
                copy(i, slot).start()
                return c

            n = 2 * h // ROWS
            lax.fori_loop(0, n, chunk, 0)
            for i in range(n - SLOTS, n):
                copy(i, i % SLOTS).wait()


def main(coarse, d4, d3, d2, d1, rafter, rbefore, cafter, cbefore):
    vmem = pl.BlockSpec(memory_space=pltpu.VMEM)
    return pl.pallas_call(
        main_kernel,
        in_specs=[vmem] * 9,
        out_specs=pl.BlockSpec(memory_space=pl.ANY),
        out_shape=jax.ShapeDtypeStruct((1024, 2048), f32),
        scratch_shapes=[
            pltpu.VMEM((8, RW), f32),
            pltpu.VMEM((8 * CG, 128), f32),
            pltpu.VMEM((9, 1040, 128), f32),
            pltpu.VMEM((9, 1040, 128), f32),
            pltpu.VMEM((144, 384), f32),
            pltpu.VMEM((272, 640), f32),
            pltpu.VMEM((528, 1152), f32),
            pltpu.VMEM((512, 256), bf16),
            pltpu.VMEM((SLOTS, ROWS, 2048), f32),
            pltpu.SemaphoreType.DMA((SLOTS,)),
        ],
        compiler_params=pltpu.CompilerParams(vmem_limit_bytes=40 << 20),
        name="synthesis",
    )(coarse, d4, d3, d2, d1, rafter, rbefore, cafter, cbefore)


def per_device(coarse, detail4, detail3, detail2, detail1):
    details = (detail1, detail2, detail3, detail4)

    def swap(to_prev, to_next, axis):
        n = lax.axis_size(axis)
        down = [((i + 1) % n, i) for i in range(n)]
        up = [(i, (i + 1) % n) for i in range(n)]
        return lax.ppermute(to_prev, axis, down), lax.ppermute(to_next, axis, up)

    rafter, rbefore = swap(*row_pack(coarse, details), "rows")
    cafter, cbefore = swap(*col_pack(coarse, details, rafter, rbefore), "cols")
    return main(coarse, detail4, detail3, detail2, detail1, rafter, rbefore, cafter, cbefore)


def solution(mesh):
    return jax.shard_map(
        per_device,
        mesh=mesh,
        in_specs=(
            P("rows", "cols"),
            P(None, "rows", "cols"),
            P(None, "rows", "cols"),
            P(None, "rows", "cols"),
            P(None, "rows", "cols"),
        ),
        out_specs=P("rows", "cols"),
        check_vma=False,
    )
```

```python
import functools

import jax
import jax.numpy as jnp
from jax import lax
from jax.experimental import pallas as pl
from jax.experimental.pallas import tpu as pltpu
from jax.sharding import PartitionSpec as P

lift_alpha = -1.586134342059924
lift_beta = -0.052980118572961
lift_gamma = 0.882911075530934
lift_delta = 0.443506852043971
lift_scale = 1.149604398860241
SQ = lift_scale * lift_scale

H = (512, 256, 128, 64)
W = (1024, 512, 256, 128)
PLANES = tuple((k, p) for k in range(4) for p in range(3)) + ((3, 3),)
ROFF = []
COFF = []
_r = _c = 0
for _k, _p in PLANES:
    ROFF.append(_r)
    COFF.append(_c)
    _r += W[_k]
    _c += H[_k] // 8
RW = _r
OWN = _c
CG = OWN + 13
HALF = RW // 2
PK = -(-CG // 32)
CORNER = OWN // 32

f32 = jnp.float32
bf16 = jnp.bfloat16
VMEM = pl.BlockSpec(memory_space=pltpu.VMEM)
HBM = pl.BlockSpec(memory_space=pltpu.HBM)
SMALL = pltpu.CompilerParams(vmem_limit_bytes=6 << 20)


def iota(shape, dim):
    return lax.broadcasted_iota(jnp.int32, shape, dim)


def col_group(n, g):
    return OWN + n if g == H[PLANES[n][0]] // 8 else COFF[n] + g


def row_pack_kernel(d1, d2, d3, d4, coarse, up, down, top, bot, sems):
    copies = []
    for n, (k, p) in enumerate(PLANES):
        src = coarse if p == 3 else (d1, d2, d3, d4)[k].at[p]
        lanes = pl.ds(ROFF[n], W[k])
        copies.append(pltpu.make_async_copy(src.at[pl.ds(0, 8), :], top.at[:, lanes], sems.at[2 * n]))
        copies.append(
            pltpu.make_async_copy(src.at[pl.ds(H[k] - 8, 8), :], bot.at[:, lanes], sems.at[2 * n + 1])
        )
    for c in copies:
        c.start()
    for c in copies:
        c.wait()
    low = iota((8, HALF), 0) < 4
    up[...] = jnp.where(low, top[:, :HALF], pltpu.roll(top[:, HALF:], 4, 0))
    down[...] = jnp.where(low, pltpu.roll(bot[:, :HALF], 4, 0), bot[:, HALF:])


def row_pack(coarse, details):
    out = jax.ShapeDtypeStruct((8, HALF), f32)
    return pl.pallas_call(
        row_pack_kernel,
        in_specs=[HBM] * 5,
        out_specs=[VMEM] * 2,
        out_shape=[out, out],
        scratch_shapes=[
            pltpu.VMEM((8, RW), f32),
            pltpu.VMEM((8, RW), f32),
            pltpu.SemaphoreType.DMA((26,)),
        ],
        compiler_params=SMALL,
        name="row_pack",
    )(*(pltpu.with_memory_space_constraint(x, pltpu.HBM) for x in (*details, coarse)))


def row_unpack(after, before):
    low = iota(after.shape, 0) < 4
    first = jnp.where(low, after, pltpu.roll(before, 4, 0))
    second = jnp.where(low, pltpu.roll(after, 4, 0), before)
    return first, second


def place(edges, lacc, racc):
    lane = iota((8, 128), 1)
    for q, e in edges:
        m, j = divmod(q, 32)
        nxt = (4 * j + 4) % 128
        e = e()
        if nxt:
            e = pltpu.roll(e, nxt, 1)
        lacc[m] = jnp.where((lane >= nxt) & (lane < nxt + 4), e, lacc[m])
        racc[m] = jnp.where((lane >= 4 * j) & (lane < 4 * j + 4), e, racc[m])


def col_pack_kernel(d1, d2, d3, d4, coarse, _, left_out, right_out):
    details = (d1, d2, d3, d4)
    lane = iota((8, 128), 1)

    def edge(n, g):
        k, p = PLANES[n]
        rows = slice(8 * g, 8 * g + 8)
        if p == 3:
            return coarse[rows, :]
        lo, hi = details[k][p, rows, :128], details[k][p, rows, W[k] - 128 :]
        return jnp.where(lane < 64, lo, hi)

    order = {}
    for n, (k, p) in enumerate(PLANES):
        for g in range(H[k] // 8):
            order[COFF[n] + g] = functools.partial(edge, n, g)
    lacc = {m: jnp.zeros((8, 128), f32) for m in range(PK)}
    racc = {m: jnp.zeros((8, 128), f32) for m in range(PK)}
    place([(q, order[q]) for j in range(32) for q in range(j, OWN, 32)], lacc, racc)
    for m in range(PK):
        left_out[8 * m : 8 * m + 8, :] = lacc[m]
        right_out[8 * m : 8 * m + 8, :] = racc[m]


def corner_kernel(left, right, after, before, left_out, right_out):
    first, second = row_unpack(after[...], before[...])
    lane = iota((8, 128), 1)
    left_out[...] = left[...]
    right_out[...] = right[...]

    def piece(o):
        return first[:, o : o + 128] if o < HALF else second[:, o - HALF : o - HALF + 128]

    def edge(n):
        return jnp.where(lane < 64, piece(ROFF[n]), piece(ROFF[n] + W[PLANES[n][0]] - 128))

    rows = slice(8 * CORNER, 8 * CORNER + 8)
    lacc, racc = {CORNER: left[rows, :]}, {CORNER: right[rows, :]}
    place([(OWN + n, functools.partial(edge, n)) for n in range(13)], lacc, racc)
    left_out[rows, :] = lacc[CORNER]
    right_out[rows, :] = racc[CORNER]


def col_pack(coarse, details, after_this):
    out = jax.ShapeDtypeStruct((8 * PK, 128), f32)
    return pl.pallas_call(
        col_pack_kernel,
        in_specs=[VMEM] * 5 + [HBM],
        out_specs=[VMEM] * 2,
        out_shape=[out, out],
        compiler_params=SMALL,
        name="col_pack",
    )(*details, coarse, after_this)


def corners(left, right, after, before):
    out = jax.ShapeDtypeStruct((8 * PK, 128), f32)
    return pl.pallas_call(
        corner_kernel,
        in_specs=[VMEM] * 4,
        out_specs=[VMEM] * 2,
        out_shape=[out, out],
        compiler_params=SMALL,
        name="corners",
    )(left, right, after, before)


def vertical(load_s, load_r, groups, store_s, store_r, tmp):
    sub = iota((8, 128), 0)
    first, last = sub == 0, sub == 7

    def cached(f):
        memo = {}

        def get(g):
            g = g % groups
            if g not in memo:
                memo[g] = f(g)
            return memo[g]

        return get

    def kept(f, ref):
        def make(g):
            x = f(g)
            ref[8 * g : 8 * g + 8, :] = x
            return x

        return cached(make)

    def prev_of(x, ref):
        def get(g):
            a, b = x(g - 1), x(g)
            if g:
                return ref[8 * g - 1 : 8 * g + 7, :]
            return jnp.where(first, pltpu.roll(a, 1, 0), pltpu.roll(b, 1, 0))

        return get

    def next_of(x, ref):
        def get(g):
            a, b = x(g), x(g + 1)
            if g < groups - 1:
                return ref[8 * g + 1 : 8 * g + 9, :]
            return jnp.where(last, pltpu.roll(b, 7, 0), pltpu.roll(a, 7, 0))

        return get

    s = cached(load_s)
    r = kept(load_r, tmp.at[0])
    rp = prev_of(r, tmp.at[0])
    s1 = kept(lambda g: s(g) - lift_delta * (r(g) + rp(g)), tmp.at[1])
    s1n = next_of(s1, tmp.at[1])
    r1 = kept(lambda g: r(g) - lift_gamma * (s1(g) + s1n(g)), tmp.at[2])
    r1p = prev_of(r1, tmp.at[2])
    s2 = kept(lambda g: s1(g) - lift_beta * (r1(g) + r1p(g)), tmp.at[3])
    s2n = next_of(s2, tmp.at[3])
    r2 = cached(lambda g: r1(g) - lift_alpha * (s2(g) + s2n(g)))
    for g in range(groups):
        store_s(g, s2(g))
        store_r(g, r2(g))


def lanes_of(b):
    return pl.ds(128 * b if isinstance(b, int) else pl.multiple_of(b * 128, 128), 128)


def interleaved_store(ref, odd, skip):
    def put(g, x):
        if g != skip:
            ref[pl.ds(16 * g + odd, 8, 2), :] = x

    return put


def high_columns(k, load, ref, tmp):
    groups = H[k] // 8 + 1
    skip = groups - 1 if k == 0 else -1
    vertical(
        lambda g: load(0, g),
        lambda g: load(2, g) * (1.0 / SQ),
        groups,
        interleaved_store(ref, 0, skip),
        interleaved_store(ref, 1, skip),
        tmp,
    )


def loop(n, f):
    if n == 1:
        f(0)
    else:
        lax.fori_loop(0, n, lambda i, c: (f(i), c)[1], 0)


def detail_kernel(d1, d2, d3, d4, after, before, v1, v2, v3, v4, xr, tmp):
    details, vs = (d1, d2, d3, d4), (v1, v2, v3, v4)
    first, second = row_unpack(after[...], before[...])
    xr[:, :HALF] = first
    xr[:, HALF:] = second
    for k in (3, 2, 1, 0):
        def columns(b, k=k):
            def load(p, g):
                if g == H[k] // 8:
                    o = ROFF[3 * k + p]
                    if isinstance(b, int):
                        return xr[:, o + 128 * b : o + 128 * b + 128]
                    return xr[:, pl.ds(pl.multiple_of(o + b * 128, 128), 128)]
                return details[k][p, 8 * g : 8 * g + 8, lanes_of(b)]

            high_columns(k, load, vs[k].at[b], tmp)

        loop(W[k] // 128, columns)


def detail_columns(details, after, before):
    outs = [jax.ShapeDtypeStruct((W[k] // 128, 2 * H[k] + 16, 128), f32) for k in range(4)]
    outs.append(jax.ShapeDtypeStruct((8, RW), f32))
    return pl.pallas_call(
        detail_kernel,
        in_specs=[VMEM] * 6,
        out_specs=[VMEM] * 5,
        out_shape=outs,
        scratch_shapes=[pltpu.VMEM((4, 520, 128), f32)],
        compiler_params=SMALL,
        name="detail_columns",
    )(*details, after, before)


def horizontal(s, r):
    n = s.shape[1]
    s = s - lift_delta * (r + pltpu.roll(r, 1, 1))
    r = r - lift_gamma * (s + pltpu.roll(s, n - 1, 1))
    s = s - lift_beta * (r + pltpu.roll(r, 1, 1))
    r = r - lift_alpha * (s + pltpu.roll(s, n - 1, 1))
    return s, r


def interleave(s, r, blocks, perm):
    rows = s.shape[0]
    x = jnp.concatenate(
        [
            jnp.concatenate([s[:, 128 * b : 128 * b + 128], r[:, 128 * b : 128 * b + 128]], axis=1)
            for b in range(blocks)
        ],
        axis=0,
    )
    hi = x.astype(bf16)
    lo = (x - hi.astype(f32)).astype(bf16)
    y = jnp.dot(jnp.concatenate([hi, lo], axis=1), perm, preferred_element_type=f32)
    return [y[rows * b : rows * b + rows, :] for b in range(blocks)]


CHUNK = (128, 264, 272, 144)
SLOTS = 3


def main_kernel(
    coarse, d4, d3, d2, d1, v1, v2, v3, v4, xr, cafter, cbefore, out,
    xc, u, vx, l3, l2, l1, perm, stage, tmp, sems,
):
    details, vs = (d1, d2, d3, d4), (v1, v2, v3, v4)
    lows = (l1, l2, l3)
    lane = iota((8, 128), 1)

    even = (iota((8 * PK, 128), 1) % 8) < 4
    aft, bef = cafter[...], cbefore[...]
    comb = (jnp.where(even, bef, aft), jnp.where(even, aft, bef))
    keep = (lane < 4) | (lane >= 124)
    for q in range(CG):
        m, j = divmod(q, 32)
        t = comb[j % 2][8 * m : 8 * m + 8, :]
        shift = (124 - 4 * j) % 128
        if shift:
            t = pltpu.roll(t, shift, 1)
        xc[8 * q : 8 * q + 8, :] = jnp.where(keep, t, 0.0)

    row = iota((512, 256), 0) % 256
    col = iota((512, 256), 1)
    target = jnp.where(row < 128, 2 * row, 2 * row - 255)
    perm[...] = jnp.where(col == target, 1.0, 0.0).astype(bf16)

    for k in (3, 2, 1, 0):
        h, w = H[k], W[k]
        groups, blocks = h // 8 + 1, w // 128
        skip = groups - 1 if k == 0 else -1

        def load(p, g, b, k=k, groups=groups, blocks=blocks):
            n = 3 * k + p if p < 3 else 12
            rows = slice(8 * g, 8 * g + 8)
            if p == 3 and k < 3:
                return lows[k][rows, lanes_of(b)]
            if isinstance(b, int) and b == blocks:
                q = col_group(n, g)
                return xc[8 * q : 8 * q + 8, :]
            if g == groups - 1:
                if isinstance(b, int):
                    return xr[:, ROFF[n] + 128 * b : ROFF[n] + 128 * b + 128]
                return xr[:, pl.ds(pl.multiple_of(ROFF[n] + b * 128, 128), 128)]
            if p == 3:
                return coarse[rows, lanes_of(b)]
            return details[k][p, rows, lanes_of(b)]

        def columns(b, load=load, groups=groups, skip=skip):
            vertical(
                lambda g: load(3, g, b) * SQ,
                lambda g: load(1, g, b),
                groups,
                interleaved_store(u.at[b], 0, skip),
                interleaved_store(u.at[b], 1, skip),
                tmp,
            )

        loop(blocks, columns)
        columns(blocks)
        high_columns(k, lambda p, g, load=load, blocks=blocks: load(p, g, blocks), vx, tmp)

        def rows_of(at, rows, blocks=blocks, k=k):
            at = pl.ds(at, rows)
            s = jnp.concatenate([u[b, at, :] for b in range(blocks + 1)], axis=1)
            r = jnp.concatenate([vs[k][b, at, :] for b in range(blocks)] + [vx[at, :]], axis=1)
            return horizontal(s, r)

        rows = CHUNK[k]
        if k:
            low = lows[k - 1]

            def chunk(i, rows=rows, rows_of=rows_of, low=low, blocks=blocks):
                at = i * rows if isinstance(i, int) else pl.multiple_of(i * rows, 8)
                s, r = rows_of(at, rows)
                parts = interleave(s, r, blocks + 1, perm[...])
                for b in range(blocks):
                    low[pl.ds(at, rows), 256 * b : 256 * b + 256] = parts[b]
                left, right = parts[blocks][:, :128], parts[blocks][:, 128:]
                low[pl.ds(at, rows), 256 * blocks : 256 * blocks + 128] = jnp.where(
                    iota((rows, 128), 1) < 64, left, right
                )

            loop(16 * groups // rows, chunk)
            top = low[2 * h : 2 * h + 8, :]
            bottom = low[2 * h + 8 : 2 * h + 16, :]
            low[2 * h : 2 * h + 8, :] = jnp.where(iota(top.shape, 0) < 4, top, bottom)
        else:
            def copy(i, slot, rows=rows):
                return pltpu.make_async_copy(
                    stage.at[slot], out.at[pl.ds(pl.multiple_of(i * rows, 8), rows), :], sems.at[slot]
                )

            def chunk(i, rows_of=rows_of, blocks=blocks, rows=rows):
                slot = lax.rem(i, SLOTS)

                @pl.when(i >= SLOTS)
                def _():
                    copy(i - SLOTS, slot).wait()

                s, r = rows_of(pl.multiple_of(i * rows, 8), rows)
                parts = interleave(s, r, blocks, perm[...])
                for b in range(blocks):
                    stage[slot, :, 256 * b : 256 * b + 256] = parts[b]
                copy(i, slot).start()

            n = 2 * h // rows
            loop(n, chunk)
            for i in range(n - SLOTS, n):
                copy(i, i % SLOTS).wait()


def main(coarse, d4, d3, d2, d1, *rest):
    return pl.pallas_call(
        main_kernel,
        in_specs=[VMEM] * 12,
        out_specs=HBM,
        out_shape=jax.ShapeDtypeStruct((1024, 2048), f32),
        scratch_shapes=[
            pltpu.VMEM((8 * CG, 128), f32),
            pltpu.VMEM((9, 1040, 128), f32),
            pltpu.VMEM((1040, 128), f32),
            pltpu.VMEM((144, 384), f32),
            pltpu.VMEM((272, 640), f32),
            pltpu.VMEM((528, 1152), f32),
            pltpu.VMEM((512, 256), bf16),
            pltpu.VMEM((SLOTS, CHUNK[0], 2048), f32),
            pltpu.VMEM((4, 520, 128), f32),
            pltpu.SemaphoreType.DMA((SLOTS,)),
        ],
        compiler_params=pltpu.CompilerParams(vmem_limit_bytes=32 << 20),
        name="synthesis",
    )(coarse, d4, d3, d2, d1, *rest)


def per_device(coarse, detail4, detail3, detail2, detail1):
    details = (detail1, detail2, detail3, detail4)

    def swap(to_prev, to_next, axis):
        n = lax.axis_size(axis)
        down = [((i + 1) % n, i) for i in range(n)]
        up = [(i, (i + 1) % n) for i in range(n)]
        return lax.ppermute(to_prev, axis, down), lax.ppermute(to_next, axis, up)

    up, down = row_pack(coarse, details)
    rafter, rbefore = swap(up, down, "rows")
    packed = col_pack(coarse, details, up)
    cafter, cbefore = swap(*corners(*packed, rafter, rbefore), "cols")
    highs = detail_columns(details, rafter, rbefore)
    return main(coarse, detail4, detail3, detail2, detail1, *highs, cafter, cbefore)


def solution(mesh):
    return jax.shard_map(
        per_device,
        mesh=mesh,
        in_specs=(
            P("rows", "cols"),
            P(None, "rows", "cols"),
            P(None, "rows", "cols"),
            P(None, "rows", "cols"),
            P(None, "rows", "cols"),
        ),
        out_specs=P("rows", "cols"),
        check_vma=False,
    )
```

```python
import functools

import jax
import jax.numpy as jnp
from jax import lax
from jax.experimental import pallas as pl
from jax.experimental.pallas import tpu as pltpu
from jax.sharding import PartitionSpec as P

lift_alpha = -1.586134342059924
lift_beta = -0.052980118572961
lift_gamma = 0.882911075530934
lift_delta = 0.443506852043971
lift_scale = 1.149604398860241
SQ = lift_scale * lift_scale

H = (512, 256, 128, 64)
W = (1024, 512, 256, 128)
PLANES = tuple((k, p) for k in range(4) for p in range(3)) + ((3, 3),)
ROFF = []
COFF = []
_r = _c = 0
for _k, _p in PLANES:
    ROFF.append(_r)
    COFF.append(_c)
    _r += W[_k]
    _c += H[_k] // 8
RW = _r
OWN = _c
CG = OWN + 13
HALF = RW // 2
PK = -(-CG // 32)
CORNER = OWN // 32

f32 = jnp.float32
bf16 = jnp.bfloat16
VMEM = pl.BlockSpec(memory_space=pltpu.VMEM)
HBM = pl.BlockSpec(memory_space=pltpu.HBM)
ANY = pl.BlockSpec(memory_space=pl.ANY)
SMALL = pltpu.CompilerParams(vmem_limit_bytes=6 << 20)


def iota(shape, dim):
    return lax.broadcasted_iota(jnp.int32, shape, dim)


def col_group(n, g):
    return OWN + n if g == H[PLANES[n][0]] // 8 else COFF[n] + g


def row_pack_kernel(d1, d2, d3, d4, coarse, up, down, *scratch):
    sources = (d1, d2, d3, d4, coarse)
    tops, bots, sems = scratch[:5], scratch[5:10], scratch[10]
    copies = []
    for n, src in enumerate(sources):
        last = src.shape[-2] - 8
        for side, at, dst in ((0, 0, tops[n]), (1, last, bots[n])):
            rows = src.at[pl.ds(at, 8), :] if n == 4 else src.at[:, pl.ds(at, 8), :]
            copies.append(pltpu.make_async_copy(rows, dst, sems.at[2 * n + side]))
    for c in copies:
        c.start()
    for c in copies:
        c.wait()

    def line(refs):
        return jnp.concatenate([refs[k][p] if p < 3 else refs[4][...] for k, p in PLANES], axis=1)

    top, bot = line(tops), line(bots)
    low = iota((8, HALF), 0) < 4
    up[...] = jnp.where(low, top[:, :HALF], pltpu.roll(top[:, HALF:], 4, 0))
    down[...] = jnp.where(low, pltpu.roll(bot[:, :HALF], 4, 0), bot[:, HALF:])


def row_pack(coarse, details):
    out = jax.ShapeDtypeStruct((8, HALF), f32)
    edges = [pltpu.VMEM((3, 8, w), f32) for w in W] + [pltpu.VMEM((8, W[3]), f32)]
    return pl.pallas_call(
        row_pack_kernel,
        in_specs=[HBM] * 5,
        out_specs=[VMEM] * 2,
        out_shape=[out, out],
        scratch_shapes=edges + edges + [pltpu.SemaphoreType.DMA((10,))],
        compiler_params=SMALL,
        name="row_pack",
    )(*(pltpu.with_memory_space_constraint(x, pltpu.HBM) for x in (*details, coarse)))


def row_unpack(after, before):
    low = iota(after.shape, 0) < 4
    first = jnp.where(low, after, pltpu.roll(before, 4, 0))
    second = jnp.where(low, pltpu.roll(after, 4, 0), before)
    return first, second


def place(edges, lacc, racc):
    lane = iota((8, 128), 1)
    for q, e in edges:
        m, j = divmod(q, 32)
        nxt = (4 * j + 4) % 128
        e = e()
        if nxt:
            e = pltpu.roll(e, nxt, 1)
        lacc[m] = jnp.where((lane >= nxt) & (lane < nxt + 4), e, lacc[m])
        racc[m] = jnp.where((lane >= 4 * j) & (lane < 4 * j + 4), e, racc[m])


def col_pack_kernel(d1, d2, d3, d4, coarse, _, left_out, right_out):
    details = (d1, d2, d3, d4)
    lane = iota((8, 128), 1)

    def edge(n, g):
        k, p = PLANES[n]
        rows = slice(8 * g, 8 * g + 8)
        if p == 3:
            return coarse[rows, :]
        lo, hi = details[k][p, rows, :128], details[k][p, rows, W[k] - 128 :]
        return jnp.where(lane < 64, lo, hi)

    order = {}
    for n, (k, p) in enumerate(PLANES):
        for g in range(H[k] // 8):
            order[COFF[n] + g] = functools.partial(edge, n, g)
    lacc = {m: jnp.zeros((8, 128), f32) for m in range(PK)}
    racc = {m: jnp.zeros((8, 128), f32) for m in range(PK)}
    place([(q, order[q]) for j in range(32) for q in range(j, OWN, 32)], lacc, racc)
    for m in range(PK):
        left_out[8 * m : 8 * m + 8, :] = lacc[m]
        right_out[8 * m : 8 * m + 8, :] = racc[m]


def corner_kernel(left, right, after, before, _, across, within):
    odd = lax.axis_index("cols") % 2 == 1
    first, second = row_unpack(after[...], before[...])
    lane = iota((8, 128), 1)
    across[...] = jnp.where(odd, right[...], left[...])
    within[...] = jnp.where(odd, left[...], right[...])

    def piece(o):
        return first[:, o : o + 128] if o < HALF else second[:, o - HALF : o - HALF + 128]

    def edge(n):
        return jnp.where(lane < 64, piece(ROFF[n]), piece(ROFF[n] + W[PLANES[n][0]] - 128))

    rows = slice(8 * CORNER, 8 * CORNER + 8)
    lacc, racc = {CORNER: left[rows, :]}, {CORNER: right[rows, :]}
    place([(OWN + n, functools.partial(edge, n)) for n in range(13)], lacc, racc)
    across[rows, :] = jnp.where(odd, racc[CORNER], lacc[CORNER])
    within[rows, :] = jnp.where(odd, lacc[CORNER], racc[CORNER])


def col_pack(coarse, details, after_this):
    out = jax.ShapeDtypeStruct((8 * PK, 128), f32)
    return pl.pallas_call(
        col_pack_kernel,
        in_specs=[VMEM] * 5 + [HBM],
        out_specs=[VMEM] * 2,
        out_shape=[out, out],
        compiler_params=SMALL,
        name="col_pack",
    )(*details, coarse, after_this)


def corners(left, right, after, before, after_this):
    out = jax.ShapeDtypeStruct((8 * PK, 128), f32)
    return pl.pallas_call(
        corner_kernel,
        in_specs=[VMEM] * 4 + [ANY],
        out_specs=[VMEM] * 2,
        out_shape=[out, out],
        compiler_params=SMALL,
        name="corners",
    )(left, right, after, before, after_this)


def vertical(load_s, load_r, groups, store_s, store_r, tmp):
    sub = iota((8, 128), 0)
    first, last = sub == 0, sub == 7

    def cached(f):
        memo = {}

        def get(g):
            g = g % groups
            if g not in memo:
                memo[g] = f(g)
            return memo[g]

        return get

    def kept(f, ref):
        def make(g):
            x = f(g)
            ref[8 * g : 8 * g + 8, :] = x
            return x

        return cached(make)

    def prev_of(x, ref):
        def get(g):
            a, b = x(g - 1), x(g)
            if g:
                return ref[8 * g - 1 : 8 * g + 7, :]
            return jnp.where(first, pltpu.roll(a, 1, 0), pltpu.roll(b, 1, 0))

        return get

    def next_of(x, ref):
        def get(g):
            a, b = x(g), x(g + 1)
            if g < groups - 1:
                return ref[8 * g + 1 : 8 * g + 9, :]
            return jnp.where(last, pltpu.roll(b, 7, 0), pltpu.roll(a, 7, 0))

        return get

    s = cached(load_s)
    r = kept(load_r, tmp.at[0])
    rp = prev_of(r, tmp.at[0])
    s1 = kept(lambda g: s(g) - lift_delta * (r(g) + rp(g)), tmp.at[1])
    s1n = next_of(s1, tmp.at[1])
    r1 = kept(lambda g: r(g) - lift_gamma * (s1(g) + s1n(g)), tmp.at[2])
    r1p = prev_of(r1, tmp.at[2])
    s2 = kept(lambda g: s1(g) - lift_beta * (r1(g) + r1p(g)), tmp.at[3])
    s2n = next_of(s2, tmp.at[3])
    r2 = cached(lambda g: r1(g) - lift_alpha * (s2(g) + s2n(g)))
    for g in range(groups):
        store_s(g, s2(g))
        store_r(g, r2(g))


def lanes_of(b):
    return pl.ds(128 * b if isinstance(b, int) else pl.multiple_of(b * 128, 128), 128)


def interleaved_store(ref, odd, skip):
    def put(g, x):
        if g != skip:
            ref[pl.ds(16 * g + odd, 8, 2), :] = x

    return put


def high_columns(k, load, ref, tmp):
    groups = H[k] // 8 + 1
    skip = groups - 1 if k == 0 else -1
    vertical(
        lambda g: load(0, g),
        lambda g: load(2, g) * (1.0 / SQ),
        groups,
        interleaved_store(ref, 0, skip),
        interleaved_store(ref, 1, skip),
        tmp,
    )


def loop(n, f):
    if n == 1:
        f(0)
    else:
        lax.fori_loop(0, n, lambda i, c: (f(i), c)[1], 0)


def early_kernel(d1, _, v1, tmp):
    groups = H[0] // 8

    def columns(b):
        vertical(
            lambda g: d1[0, 8 * g : 8 * g + 8, lanes_of(b)],
            lambda g: d1[2, 8 * g : 8 * g + 8, lanes_of(b)] * (1.0 / SQ),
            groups,
            interleaved_store(v1.at[b], 0, -1),
            interleaved_store(v1.at[b], 1, -1),
            tmp,
        )

    loop(W[0] // 128, columns)


def early_columns(d1, after_this):
    return pl.pallas_call(
        early_kernel,
        in_specs=[VMEM, ANY],
        out_specs=VMEM,
        out_shape=jax.ShapeDtypeStruct((W[0] // 128, 2 * H[0], 128), f32),
        scratch_shapes=[pltpu.VMEM((4, 512, 128), f32)],
        compiler_params=SMALL,
        name="early_columns",
    )(d1, after_this)


def detail_kernel(d1, d2, d3, d4, after, before, early, _, v1, v2, v3, v4, xr, tmp):
    details, vs = (d1, d2, d3, d4), (v1, v2, v3, v4)
    first, second = row_unpack(after[...], before[...])
    xr[:, :HALF] = first
    xr[:, HALF:] = second
    for k in (3, 2, 1):
        def columns(b, k=k):
            def load(p, g):
                if g == H[k] // 8:
                    o = ROFF[3 * k + p]
                    if isinstance(b, int):
                        return xr[:, o + 128 * b : o + 128 * b + 128]
                    return xr[:, pl.ds(pl.multiple_of(o + b * 128, 128), 128)]
                return details[k][p, 8 * g : 8 * g + 8, lanes_of(b)]

            high_columns(k, load, vs[k].at[b], tmp)

        loop(W[k] // 128, columns)

    last = H[0] // 8 - 1
    around = (last - 1, last, last + 1, 0, 1)

    def load(p, b, i):
        g = around[i]
        if g > last:
            return xr[:, ROFF[p] + 128 * b : ROFF[p] + 128 * b + 128]
        return d1[p, 8 * g : 8 * g + 8, 128 * b : 128 * b + 128]

    def put(b, odd):
        def store(i, x):
            if i in (1, 3):
                v1[b, pl.ds(16 * around[i] + odd, 8, 2), :] = x

        return store

    for b in range(W[0] // 128):
        vertical(
            functools.partial(load, 0, b),
            lambda i, b=b: load(2, b, i) * (1.0 / SQ),
            5,
            put(b, 0),
            put(b, 1),
            tmp.at[:, pl.ds(40 * b, 40), :],
        )


def detail_columns(details, after, before, early, after_this):
    outs = [jax.ShapeDtypeStruct(early.shape, f32)]
    outs += [jax.ShapeDtypeStruct((W[k] // 128, 2 * H[k] + 16, 128), f32) for k in (1, 2, 3)]
    outs.append(jax.ShapeDtypeStruct((8, RW), f32))
    return pl.pallas_call(
        detail_kernel,
        in_specs=[VMEM] * 7 + [ANY],
        out_specs=[VMEM] * 5,
        out_shape=outs,
        input_output_aliases={6: 0},
        scratch_shapes=[pltpu.VMEM((4, 320, 128), f32)],
        compiler_params=SMALL,
        name="detail_columns",
    )(*details, after, before, early, after_this)


def interleave(s, r, blocks, perm, parts=1):
    rows = s.shape[0]
    x = jnp.concatenate(
        [
            jnp.concatenate([s[:, 128 * b : 128 * b + 128], r[:, 128 * b : 128 * b + 128]], axis=1)
            for b in range(blocks)
        ],
        axis=0,
    )
    hi = x.astype(bf16)
    lo = (x - hi.astype(f32)).astype(bf16)
    x = jnp.concatenate([hi, lo], axis=1)
    step = blocks * rows // parts // 16 * 16
    cuts = [*range(0, step * parts, step), blocks * rows]
    y = [
        jnp.dot(x[i:j, :], perm[...], preferred_element_type=f32) for i, j in zip(cuts[:-1], cuts[1:])
    ]
    y = jnp.concatenate(y, axis=0)
    return [y[rows * b : rows * b + rows, :] for b in range(blocks)]


CHUNK = (64, 88, 136, 144)
SLOTS = 4


def main_kernel(
    coarse, d4, d3, d2, d1, v1, v2, v3, v4, xr, across, within, out,
    xc, u, vx, l3, l2, l1, perm, s1, r1, s2, stage, tmp, sems,
):
    details, vs = (d1, d2, d3, d4), (v1, v2, v3, v4)
    lows = (l1, l2, l3)
    lane = iota((8, 128), 1)

    even = (iota((8 * PK, 128), 1) % 8) < 4
    odd = lax.axis_index("cols") % 2 == 1
    aft = jnp.where(odd, across[...], within[...])
    bef = jnp.where(odd, within[...], across[...])
    comb = (jnp.where(even, bef, aft), jnp.where(even, aft, bef))
    keep = (lane < 4) | (lane >= 124)
    for q in range(CG):
        m, j = divmod(q, 32)
        t = comb[j % 2][8 * m : 8 * m + 8, :]
        shift = (124 - 4 * j) % 128
        if shift:
            t = pltpu.roll(t, shift, 1)
        xc[8 * q : 8 * q + 8, :] = jnp.where(keep, t, 0.0)

    row = iota((512, 256), 0) % 256
    col = iota((512, 256), 1)
    target = jnp.where(row < 128, 2 * row, 2 * row - 255)
    perm[...] = jnp.where(col == target, 1.0, 0.0).astype(bf16)

    for k in (3, 2, 1, 0):
        h, w = H[k], W[k]
        groups, blocks = h // 8 + 1, w // 128
        skip = groups - 1 if k == 0 else -1

        def load(p, g, b, k=k, groups=groups, blocks=blocks):
            n = 3 * k + p if p < 3 else 12
            rows = slice(8 * g, 8 * g + 8)
            if p == 3 and k < 3:
                return lows[k][rows, lanes_of(b)]
            if isinstance(b, int) and b == blocks:
                q = col_group(n, g)
                return xc[8 * q : 8 * q + 8, :]
            if g == groups - 1:
                if isinstance(b, int):
                    return xr[:, ROFF[n] + 128 * b : ROFF[n] + 128 * b + 128]
                return xr[:, pl.ds(pl.multiple_of(ROFF[n] + b * 128, 128), 128)]
            if p == 3:
                return coarse[rows, lanes_of(b)]
            return details[k][p, rows, lanes_of(b)]

        def columns(b, load=load, groups=groups, skip=skip):
            vertical(
                lambda g: load(3, g, b) * SQ,
                lambda g: load(1, g, b),
                groups,
                interleaved_store(u.at[b], 0, skip),
                interleaved_store(u.at[b], 1, skip),
                tmp,
            )

        if blocks < 3:
            for b in range(blocks):
                columns(b)
        else:
            loop(blocks, columns)
        columns(blocks)
        high_columns(k, lambda p, g, load=load, blocks=blocks: load(p, g, blocks), vx, tmp)

        rows = CHUNK[k]
        count = 2 * h // rows if k == 0 else 16 * groups // rows
        width = w + 128
        kept = blocks + (k > 0)

        def at_rows(i, rows=rows):
            return pl.ds(i * rows if isinstance(i, int) else pl.multiple_of(i * rows, 8), rows)

        def slot(i):
            return i & 3

        def u_rows(i, blocks=blocks):
            return jnp.concatenate([u[b, at_rows(i), :] for b in range(blocks + 1)], axis=1)

        def v_rows(i, blocks=blocks, k=k):
            return jnp.concatenate(
                [vs[k][b, at_rows(i), :] for b in range(blocks)] + [vx[at_rows(i), :]], axis=1
            )

        def held(ref, i, rows=rows, width=width):
            return ref.at[slot(i), pl.ds(0, rows), pl.ds(0, width)]

        def step1(i, width=width):
            r = v_rows(i)
            held(s1, i)[...] = u_rows(i) - lift_delta * (r + pltpu.roll(r, 1, 1))

        def step2(i, width=width):
            x = held(s1, i)[...]
            held(r1, i)[...] = v_rows(i) - lift_gamma * (x + pltpu.roll(x, width - 1, 1))

        def step3(i):
            x = held(r1, i)[...]
            held(s2, i)[...] = held(s1, i)[...] - lift_beta * (x + pltpu.roll(x, 1, 1))

        def step4(i, k=k, rows=rows, width=width, blocks=blocks, kept=kept):
            x = held(s2, i)[...]
            y = held(r1, i)[...] - lift_alpha * (x + pltpu.roll(x, width - 1, 1))
            parts = interleave(x, y, kept, perm, 2 if isinstance(i, int) else 1)
            if k == 0:
                for b in range(blocks):
                    stage[i & (SLOTS - 1), :, 256 * b : 256 * b + 256] = parts[b]
                return
            low = lows[k - 1]
            for b in range(blocks):
                low[at_rows(i), 256 * b : 256 * b + 256] = parts[b]
            left, right = parts[blocks][:, :128], parts[blocks][:, 128:]
            low[at_rows(i), 256 * blocks : 256 * blocks + 128] = jnp.where(
                iota((rows, 128), 1) < 64, left, right
            )

        steps = (step1, step2, step3, step4)

        def turn(i, k=k, steps=steps, count=count, send=True):
            def active(j):
                return not isinstance(i, int) or 0 <= i - j < count

            if k == 0 and active(3) and send:
                if isinstance(i, int):
                    copy_out(i - 3 - SLOTS, wait=True)
                else:
                    pl.when(i - 3 >= SLOTS)(lambda: copy_out(i - 3 - SLOTS, wait=True))
            for j in reversed(range(4)):
                if active(j):
                    steps[j](i - j)
            if k == 0 and active(3) and send:
                copy_out(i - 3)

        def copy_out(i, wait=False, rows=rows):
            c = i & (SLOTS - 1)
            c = pltpu.make_async_copy(stage.at[c], out.at[at_rows(i), :], sems.at[c])
            if wait:
                c.wait()
            else:
                c.start()

        first, last = (3, count) if count > 6 else (0, 0)
        for i in range(first):
            turn(i)
        if last > first:
            lax.fori_loop(first, last, lambda i, c: (turn(i), c)[1], 0)
        if k:
            for i in range(last, count + 3):
                turn(i)
        else:
            turn(count)
            copy_out(count - 2 - SLOTS, wait=True)
            copy_out(count - 1 - SLOTS, wait=True)
            turn(count + 1, send=False)
            turn(count + 2, send=False)
            copy_out(count - 2)
            copy_out(count - 1)

        if k:
            low = lows[k - 1]
            top = low[2 * h : 2 * h + 8, :]
            bottom = low[2 * h + 8 : 2 * h + 16, :]
            low[2 * h : 2 * h + 8, :] = jnp.where(iota(top.shape, 0) < 4, top, bottom)
        else:
            for i in range(count - SLOTS, count):
                copy_out(i, wait=True)


def main(coarse, d4, d3, d2, d1, *rest):
    return pl.pallas_call(
        main_kernel,
        in_specs=[VMEM] * 12,
        out_specs=HBM,
        out_shape=jax.ShapeDtypeStruct((1024, 2048), f32),
        scratch_shapes=[
            pltpu.VMEM((8 * CG, 128), f32),
            pltpu.VMEM((9, 1040, 128), f32),
            pltpu.VMEM((1040, 128), f32),
            pltpu.VMEM((144, 384), f32),
            pltpu.VMEM((272, 640), f32),
            pltpu.VMEM((528, 1152), f32),
            pltpu.VMEM((512, 256), bf16),
            pltpu.VMEM((4, 176, 1152), f32),
            pltpu.VMEM((4, 176, 1152), f32),
            pltpu.VMEM((4, 176, 1152), f32),
            pltpu.VMEM((SLOTS, CHUNK[0], 2048), f32),
            pltpu.VMEM((4, 520, 128), f32),
            pltpu.SemaphoreType.DMA((SLOTS,)),
        ],
        compiler_params=pltpu.CompilerParams(vmem_limit_bytes=32 << 20),
        name="synthesis",
    )(coarse, d4, d3, d2, d1, *rest)


def per_device(coarse, detail4, detail3, detail2, detail1):
    details = (detail1, detail2, detail3, detail4)

    n = lax.axis_size("rows")
    up, down = row_pack(coarse, details)
    rbefore = lax.ppermute(down, "rows", [(i, (i + 1) % n) for i in range(n)])
    rafter = lax.ppermute(up, "rows", [((i + 1) % n, i) for i in range(n)])
    packed = col_pack(coarse, details, up)
    early = early_columns(detail1, packed[0])
    sent = corners(*packed, rafter, rbefore, early)
    across = exchange(sent[0], 1)
    within = exchange(sent[1], 0)
    highs = detail_columns(details, rafter, rbefore, early, sent[1])
    return main(coarse, detail4, detail3, detail2, detail1, *highs, across, within)


def exchange(x, first):
    n = lax.axis_size("cols")
    pairs = [((first + i) % n, (first + i + 1) % n) for i in range(0, n, 2)]
    return lax.ppermute(x, "cols", pairs + [(j, i) for i, j in pairs])


def solution(mesh):
    return jax.shard_map(
        per_device,
        mesh=mesh,
        in_specs=(
            P("rows", "cols"),
            P(None, "rows", "cols"),
            P(None, "rows", "cols"),
            P(None, "rows", "cols"),
            P(None, "rows", "cols"),
        ),
        out_specs=P("rows", "cols"),
        check_vma=False,
    )
```

```python
import functools

import jax
import jax.numpy as jnp
from jax import lax
from jax.experimental import pallas as pl
from jax.experimental.pallas import tpu as pltpu
from jax.sharding import PartitionSpec as P

lift_alpha = -1.586134342059924
lift_beta = -0.052980118572961
lift_gamma = 0.882911075530934
lift_delta = 0.443506852043971
lift_scale = 1.149604398860241
SQ = lift_scale * lift_scale

H = (512, 256, 128, 64)
W = (1024, 512, 256, 128)
PLANES = tuple((k, p) for k in range(4) for p in range(3)) + ((3, 3),)
ROFF = []
COFF = []
_r = _c = 0
for _k, _p in PLANES:
    ROFF.append(_r)
    COFF.append(_c)
    _r += W[_k]
    _c += H[_k] // 8
RW = _r
OWN = _c
CG = OWN + 13
HALF = RW // 2
PK = -(-CG // 32)
CORNER = OWN // 32

f32 = jnp.float32
bf16 = jnp.bfloat16
VMEM = pl.BlockSpec(memory_space=pltpu.VMEM)
HBM = pl.BlockSpec(memory_space=pltpu.HBM)
ANY = pl.BlockSpec(memory_space=pl.ANY)
SMALL = pltpu.CompilerParams(vmem_limit_bytes=6 << 20)


def iota(shape, dim):
    return lax.broadcasted_iota(jnp.int32, shape, dim)


def col_group(n, g):
    return OWN + n if g == H[PLANES[n][0]] // 8 else COFF[n] + g


def row_pack_kernel(d1, d2, d3, d4, coarse, up, down, *scratch):
    sources = (d1, d2, d3, d4, coarse)
    tops, bots, sems = scratch[:5], scratch[5:10], scratch[10]
    copies = []
    for n, src in enumerate(sources):
        last = src.shape[-2] - 8
        for side, at, dst in ((0, 0, tops[n]), (1, last, bots[n])):
            rows = src.at[pl.ds(at, 8), :] if n == 4 else src.at[:, pl.ds(at, 8), :]
            copies.append(pltpu.make_async_copy(rows, dst, sems.at[2 * n + side]))
    for c in copies:
        c.start()
    for c in copies:
        c.wait()

    def line(refs):
        return jnp.concatenate([refs[k][p] if p < 3 else refs[4][...] for k, p in PLANES], axis=1)

    top, bot = line(tops), line(bots)
    low = iota((8, HALF), 0) < 4
    up[...] = jnp.where(low, top[:, :HALF], pltpu.roll(top[:, HALF:], 4, 0))
    down[...] = jnp.where(low, pltpu.roll(bot[:, :HALF], 4, 0), bot[:, HALF:])


def row_pack(coarse, details):
    out = jax.ShapeDtypeStruct((8, HALF), f32)
    edges = [pltpu.VMEM((3, 8, w), f32) for w in W] + [pltpu.VMEM((8, W[3]), f32)]
    return pl.pallas_call(
        row_pack_kernel,
        in_specs=[HBM] * 5,
        out_specs=[VMEM] * 2,
        out_shape=[out, out],
        scratch_shapes=edges + edges + [pltpu.SemaphoreType.DMA((10,))],
        compiler_params=SMALL,
        name="row_pack",
    )(*(pltpu.with_memory_space_constraint(x, pltpu.HBM) for x in (*details, coarse)))


def row_unpack(after, before):
    low = iota(after.shape, 0) < 4
    first = jnp.where(low, after, pltpu.roll(before, 4, 0))
    second = jnp.where(low, pltpu.roll(after, 4, 0), before)
    return first, second


def place(edges, lacc, racc):
    lane = iota((8, 128), 1)
    for q, e in edges:
        m, j = divmod(q, 32)
        nxt = (4 * j + 4) % 128
        e = e()
        if nxt:
            e = pltpu.roll(e, nxt, 1)
        lacc[m] = jnp.where((lane >= nxt) & (lane < nxt + 4), e, lacc[m])
        racc[m] = jnp.where((lane >= 4 * j) & (lane < 4 * j + 4), e, racc[m])


def col_pack_kernel(d1, d2, d3, d4, coarse, _, left_out, right_out):
    details = (d1, d2, d3, d4)
    lane = iota((8, 128), 1)

    def edge(n, g):
        k, p = PLANES[n]
        rows = slice(8 * g, 8 * g + 8)
        if p == 3:
            return coarse[rows, :]
        lo, hi = details[k][p, rows, :128], details[k][p, rows, W[k] - 128 :]
        return jnp.where(lane < 64, lo, hi)

    order = {}
    for n, (k, p) in enumerate(PLANES):
        for g in range(H[k] // 8):
            order[COFF[n] + g] = functools.partial(edge, n, g)
    lacc = {m: jnp.zeros((8, 128), f32) for m in range(PK)}
    racc = {m: jnp.zeros((8, 128), f32) for m in range(PK)}
    place([(q, order[q]) for j in range(32) for q in range(j, OWN, 32)], lacc, racc)
    for m in range(PK):
        left_out[8 * m : 8 * m + 8, :] = lacc[m]
        right_out[8 * m : 8 * m + 8, :] = racc[m]


def corner_kernel(left, right, after, before, _, across, within):
    odd = lax.axis_index("cols") % 2 == 1
    first, second = row_unpack(after[...], before[...])
    lane = iota((8, 128), 1)
    across[...] = jnp.where(odd, right[...], left[...])
    within[...] = jnp.where(odd, left[...], right[...])

    def piece(o):
        return first[:, o : o + 128] if o < HALF else second[:, o - HALF : o - HALF + 128]

    def edge(n):
        return jnp.where(lane < 64, piece(ROFF[n]), piece(ROFF[n] + W[PLANES[n][0]] - 128))

    rows = slice(8 * CORNER, 8 * CORNER + 8)
    lacc, racc = {CORNER: left[rows, :]}, {CORNER: right[rows, :]}
    place([(OWN + n, functools.partial(edge, n)) for n in range(13)], lacc, racc)
    across[rows, :] = jnp.where(odd, racc[CORNER], lacc[CORNER])
    within[rows, :] = jnp.where(odd, lacc[CORNER], racc[CORNER])


def col_pack(coarse, details, after_this):
    out = jax.ShapeDtypeStruct((8 * PK, 128), f32)
    return pl.pallas_call(
        col_pack_kernel,
        in_specs=[VMEM] * 5 + [HBM],
        out_specs=[VMEM] * 2,
        out_shape=[out, out],
        compiler_params=SMALL,
        name="col_pack",
    )(*details, coarse, after_this)


def corners(left, right, after, before, after_this):
    out = jax.ShapeDtypeStruct((8 * PK, 128), f32)
    return pl.pallas_call(
        corner_kernel,
        in_specs=[VMEM] * 4 + [ANY],
        out_specs=[VMEM] * 2,
        out_shape=[out, out],
        compiler_params=SMALL,
        name="corners",
    )(left, right, after, before, after_this)


def vertical(load_s, load_r, groups, store_s, store_r):
    sub = iota((8, 128), 0)
    first, last = sub == 0, sub == 7

    def cached(f):
        memo = {}

        def get(g):
            g = g % groups
            if g not in memo:
                memo[g] = f(g)
            return memo[g]

        return get

    def prev_of(x):
        turned = cached(lambda g: pltpu.roll(x(g), 1, 0))
        return lambda g: jnp.where(first, turned(g - 1), turned(g))

    def next_of(x):
        turned = cached(lambda g: pltpu.roll(x(g), 7, 0))
        return lambda g: jnp.where(last, turned(g + 1), turned(g))

    s, r = cached(load_s), cached(load_r)
    rp = prev_of(r)
    s1 = cached(lambda g: s(g) - lift_delta * (r(g) + rp(g)))
    s1n = next_of(s1)
    r1 = cached(lambda g: r(g) - lift_gamma * (s1(g) + s1n(g)))
    r1p = prev_of(r1)
    s2 = cached(lambda g: s1(g) - lift_beta * (r1(g) + r1p(g)))
    s2n = next_of(s2)
    r2 = cached(lambda g: r1(g) - lift_alpha * (s2(g) + s2n(g)))
    for g in range(groups):
        store_s(g, s2(g))
        store_r(g, r2(g))


def lanes_of(b):
    return pl.ds(128 * b if isinstance(b, int) else pl.multiple_of(b * 128, 128), 128)


def interleaved_store(ref, odd, skip):
    def put(g, x):
        if g != skip:
            ref[pl.ds(16 * g + odd, 8, 2), :] = x

    return put


def high_columns(k, load, ref):
    groups = H[k] // 8 + 1
    skip = groups - 1 if k == 0 else -1
    vertical(
        lambda g: load(0, g),
        lambda g: load(2, g) * (1.0 / SQ),
        groups,
        interleaved_store(ref, 0, skip),
        interleaved_store(ref, 1, skip),
    )


def loop(n, f):
    if n == 1:
        f(0)
    else:
        lax.fori_loop(0, n, lambda i, c: (f(i), c)[1], 0)


def early_kernel(d1, _, v1):
    groups = H[0] // 8

    def columns(b):
        vertical(
            lambda g: d1[0, 8 * g : 8 * g + 8, lanes_of(b)],
            lambda g: d1[2, 8 * g : 8 * g + 8, lanes_of(b)] * (1.0 / SQ),
            groups,
            interleaved_store(v1.at[b], 0, -1),
            interleaved_store(v1.at[b], 1, -1),
        )

    loop(W[0] // 128, columns)


def early_columns(d1, after_this):
    return pl.pallas_call(
        early_kernel,
        in_specs=[VMEM, ANY],
        out_specs=VMEM,
        out_shape=jax.ShapeDtypeStruct((W[0] // 128, 2 * H[0], 128), f32),
        compiler_params=SMALL,
        name="early_columns",
    )(d1, after_this)


def detail_kernel(d1, d2, d3, d4, after, before, early, _, v1, v2, v3, v4, xr):
    details, vs = (d1, d2, d3, d4), (v1, v2, v3, v4)
    first, second = row_unpack(after[...], before[...])
    xr[:, :HALF] = first
    xr[:, HALF:] = second
    for k in (3, 2, 1):
        def columns(b, k=k):
            def load(p, g):
                if g == H[k] // 8:
                    o = ROFF[3 * k + p]
                    if isinstance(b, int):
                        return xr[:, o + 128 * b : o + 128 * b + 128]
                    return xr[:, pl.ds(pl.multiple_of(o + b * 128, 128), 128)]
                return details[k][p, 8 * g : 8 * g + 8, lanes_of(b)]

            high_columns(k, load, vs[k].at[b])

        loop(W[k] // 128, columns)

    last = H[0] // 8 - 1
    around = (last - 1, last, last + 1, 0, 1)

    def load(p, b, i):
        g = around[i]
        if g > last:
            return xr[:, ROFF[p] + 128 * b : ROFF[p] + 128 * b + 128]
        return d1[p, 8 * g : 8 * g + 8, 128 * b : 128 * b + 128]

    def put(b, odd):
        def store(i, x):
            if i in (1, 3):
                v1[b, pl.ds(16 * around[i] + odd, 8, 2), :] = x

        return store

    for b in range(W[0] // 128):
        vertical(
            functools.partial(load, 0, b),
            lambda i, b=b: load(2, b, i) * (1.0 / SQ),
            5,
            put(b, 0),
            put(b, 1),
        )


def detail_columns(details, after, before, early, after_this):
    outs = [jax.ShapeDtypeStruct(early.shape, f32)]
    outs += [jax.ShapeDtypeStruct((W[k] // 128, 2 * H[k] + 16, 128), f32) for k in (1, 2, 3)]
    outs.append(jax.ShapeDtypeStruct((8, RW), f32))
    return pl.pallas_call(
        detail_kernel,
        in_specs=[VMEM] * 7 + [ANY],
        out_specs=[VMEM] * 5,
        out_shape=outs,
        input_output_aliases={6: 0},
        compiler_params=SMALL,
        name="detail_columns",
    )(*details, after, before, early, after_this)


def interleave(s, r, blocks, perm, parts=1):
    rows = s.shape[0]
    x = jnp.concatenate(
        [
            jnp.concatenate([s[:, 128 * b : 128 * b + 128], r[:, 128 * b : 128 * b + 128]], axis=1)
            for b in range(blocks)
        ],
        axis=0,
    )
    hi = x.astype(bf16)
    lo = (x - hi.astype(f32)).astype(bf16)
    x = jnp.concatenate([hi, lo], axis=1)
    step = blocks * rows // parts // 16 * 16
    cuts = [*range(0, step * parts, step), blocks * rows]
    y = [
        jnp.dot(x[i:j, :], perm[...], preferred_element_type=f32) for i, j in zip(cuts[:-1], cuts[1:])
    ]
    y = jnp.concatenate(y, axis=0)
    return [y[rows * b : rows * b + rows, :] for b in range(blocks)]


CHUNK = (128, 88, 136, 144)
SLOTS = 4


def main_kernel(
    coarse, d4, d3, d2, d1, v1, v2, v3, v4, xr, across, within, out,
    comb, u, vx, l3, l2, l1, perm, s1, r1, s2, stage, sems,
):
    details, vs = (d1, d2, d3, d4), (v1, v2, v3, v4)
    lows = (l1, l2, l3)
    lane = iota((8, 128), 1)

    even = (iota((8 * PK, 128), 1) % 8) < 4
    odd = lax.axis_index("cols") % 2 == 1
    aft = jnp.where(odd, across[...], within[...])
    bef = jnp.where(odd, within[...], across[...])
    comb[0] = jnp.where(even, bef, aft)
    comb[1] = jnp.where(even, aft, bef)
    keep = (lane < 4) | (lane >= 124)

    def halo_column(q):
        m, j = divmod(q, 32)
        t = comb[j % 2, 8 * m : 8 * m + 8, :]
        shift = (124 - 4 * j) % 128
        if shift:
            t = pltpu.roll(t, shift, 1)
        return jnp.where(keep, t, 0.0)

    row = iota((512, 256), 0) % 256
    col = iota((512, 256), 1)
    target = jnp.where(row < 128, 2 * row, 2 * row - 255)
    perm[...] = jnp.where(col == target, 1.0, 0.0).astype(bf16)

    for k in (3, 2, 1, 0):
        h, w = H[k], W[k]
        groups, blocks = h // 8 + 1, w // 128
        skip = groups - 1 if k == 0 else -1

        def load(p, g, b, k=k, groups=groups, blocks=blocks):
            n = 3 * k + p if p < 3 else 12
            rows = slice(8 * g, 8 * g + 8)
            if p == 3 and k < 3:
                return lows[k][rows, lanes_of(b)]
            if isinstance(b, int) and b == blocks:
                return halo_column(col_group(n, g))
            if g == groups - 1:
                if isinstance(b, int):
                    return xr[:, ROFF[n] + 128 * b : ROFF[n] + 128 * b + 128]
                return xr[:, pl.ds(pl.multiple_of(ROFF[n] + b * 128, 128), 128)]
            if p == 3:
                return coarse[rows, lanes_of(b)]
            return details[k][p, rows, lanes_of(b)]

        def columns(b, load=load, groups=groups, skip=skip):
            vertical(
                lambda g: load(3, g, b) * SQ,
                lambda g: load(1, g, b),
                groups,
                interleaved_store(u.at[b], 0, skip),
                interleaved_store(u.at[b], 1, skip),
            )

        if blocks < 3:
            for b in range(blocks):
                columns(b)
        else:
            loop(blocks, columns)
        columns(blocks)
        high_columns(k, lambda p, g, load=load, blocks=blocks: load(p, g, blocks), vx)

        rows = CHUNK[k]
        count = 2 * h // rows if k == 0 else 16 * groups // rows
        width = w + 128
        kept = blocks + (k > 0)

        def at_rows(i, rows=rows):
            return pl.ds(i * rows if isinstance(i, int) else pl.multiple_of(i * rows, 8), rows)

        def slot(i):
            return i & 3

        def u_rows(i, blocks=blocks):
            return jnp.concatenate([u[b, at_rows(i), :] for b in range(blocks + 1)], axis=1)

        def v_rows(i, blocks=blocks, k=k):
            return jnp.concatenate(
                [vs[k][b, at_rows(i), :] for b in range(blocks)] + [vx[at_rows(i), :]], axis=1
            )

        def held(ref, i, rows=rows, width=width):
            return ref.at[slot(i), pl.ds(0, rows), pl.ds(0, width)]

        def step1(i, width=width):
            r = v_rows(i)
            held(s1, i)[...] = u_rows(i) - lift_delta * (r + pltpu.roll(r, 1, 1))

        def step2(i, width=width):
            x = held(s1, i)[...]
            held(r1, i)[...] = v_rows(i) - lift_gamma * (x + pltpu.roll(x, width - 1, 1))

        def step3(i):
            x = held(r1, i)[...]
            held(s2, i)[...] = held(s1, i)[...] - lift_beta * (x + pltpu.roll(x, 1, 1))

        def step4(i, k=k, rows=rows, width=width, blocks=blocks, kept=kept):
            x = held(s2, i)[...]
            y = held(r1, i)[...] - lift_alpha * (x + pltpu.roll(x, width - 1, 1))
            parts = interleave(x, y, kept, perm, 2 if isinstance(i, int) else 1)
            if k == 0:
                for b in range(blocks):
                    stage[i & (SLOTS - 1), :, 256 * b : 256 * b + 256] = parts[b]
                return
            low = lows[k - 1]
            for b in range(blocks):
                low[at_rows(i), 256 * b : 256 * b + 256] = parts[b]
            left, right = parts[blocks][:, :128], parts[blocks][:, 128:]
            low[at_rows(i), 256 * blocks : 256 * blocks + 128] = jnp.where(
                iota((rows, 128), 1) < 64, left, right
            )

        steps = (step1, step2, step3, step4)

        def turn(i, k=k, steps=steps, count=count, send=True):
            def active(j):
                return not isinstance(i, int) or 0 <= i - j < count

            if k == 0 and active(3) and send:
                if isinstance(i, int):
                    copy_out(i - 3 - SLOTS, wait=True)
                else:
                    pl.when(i - 3 >= SLOTS)(lambda: copy_out(i - 3 - SLOTS, wait=True))
            for j in reversed(range(4)):
                if active(j):
                    steps[j](i - j)
            if k == 0 and active(3) and send:
                copy_out(i - 3)

        def copy_out(i, wait=False, rows=rows):
            c = i & (SLOTS - 1)
            c = pltpu.make_async_copy(stage.at[c], out.at[at_rows(i), :], sems.at[c])
            if wait:
                c.wait()
            else:
                c.start()

        first, last = (3, count) if count > 6 else (0, 0)
        for i in range(first):
            turn(i)
        if last > first:
            lax.fori_loop(first, last, lambda i, c: (turn(i), c)[1], 0)
        if k:
            for i in range(last, count + 3):
                turn(i)
        else:
            turn(count)
            copy_out(count - 2 - SLOTS, wait=True)
            copy_out(count - 1 - SLOTS, wait=True)
            turn(count + 1, send=False)
            turn(count + 2, send=False)
            copy_out(count - 2)
            copy_out(count - 1)

        if k:
            low = lows[k - 1]
            top = low[2 * h : 2 * h + 8, :]
            bottom = low[2 * h + 8 : 2 * h + 16, :]
            low[2 * h : 2 * h + 8, :] = jnp.where(iota(top.shape, 0) < 4, top, bottom)
        else:
            for i in range(count - SLOTS, count):
                copy_out(i, wait=True)


def main(coarse, d4, d3, d2, d1, *rest):
    return pl.pallas_call(
        main_kernel,
        in_specs=[VMEM] * 12,
        out_specs=HBM,
        out_shape=jax.ShapeDtypeStruct((1024, 2048), f32),
        scratch_shapes=[
            pltpu.VMEM((2, 8 * PK, 128), f32),
            pltpu.VMEM((9, 1040, 128), f32),
            pltpu.VMEM((1040, 128), f32),
            pltpu.VMEM((144, 384), f32),
            pltpu.VMEM((272, 640), f32),
            pltpu.VMEM((528, 1152), f32),
            pltpu.VMEM((512, 256), bf16),
            pltpu.VMEM((4, 176, 1152), f32),
            pltpu.VMEM((4, 176, 1152), f32),
            pltpu.VMEM((4, 176, 1152), f32),
            pltpu.VMEM((SLOTS, CHUNK[0], 2048), f32),
            pltpu.SemaphoreType.DMA((SLOTS,)),
        ],
        compiler_params=pltpu.CompilerParams(vmem_limit_bytes=32 << 20),
        name="synthesis",
    )(coarse, d4, d3, d2, d1, *rest)


def per_device(coarse, detail4, detail3, detail2, detail1):
    details = (detail1, detail2, detail3, detail4)

    n = lax.axis_size("rows")
    up, down = row_pack(coarse, details)
    rbefore = lax.ppermute(down, "rows", [(i, (i + 1) % n) for i in range(n)])
    rafter = lax.ppermute(up, "rows", [((i + 1) % n, i) for i in range(n)])
    packed = col_pack(coarse, details, up)
    early = early_columns(detail1, packed[0])
    sent = corners(*packed, rafter, rbefore, early)
    across = exchange(sent[0], 1)
    within = exchange(sent[1], 0)
    highs = detail_columns(details, rafter, rbefore, early, sent[1])
    return main(coarse, detail4, detail3, detail2, detail1, *highs, across, within)


def exchange(x, first):
    n = lax.axis_size("cols")
    pairs = [((first + i) % n, (first + i + 1) % n) for i in range(0, n, 2)]
    return lax.ppermute(x, "cols", pairs + [(j, i) for i, j in pairs])


def solution(mesh):
    return jax.shard_map(
        per_device,
        mesh=mesh,
        in_specs=(
            P("rows", "cols"),
            P(None, "rows", "cols"),
            P(None, "rows", "cols"),
            P(None, "rows", "cols"),
            P(None, "rows", "cols"),
        ),
        out_specs=P("rows", "cols"),
        check_vma=False,
    )
```

```python
import functools

import jax
import jax.numpy as jnp
from jax import lax
from jax.experimental import pallas as pl
from jax.experimental.pallas import tpu as pltpu
from jax.sharding import PartitionSpec as P

lift_alpha = -1.586134342059924
lift_beta = -0.052980118572961
lift_gamma = 0.882911075530934
lift_delta = 0.443506852043971
lift_scale = 1.149604398860241
SQ = lift_scale * lift_scale

H = (512, 256, 128, 64)
W = (1024, 512, 256, 128)
PLANES = tuple((k, p) for k in range(4) for p in range(3)) + ((3, 3),)
ROFF = []
COFF = []
_r = _c = 0
for _k, _p in PLANES:
    ROFF.append(_r)
    COFF.append(_c)
    _r += W[_k]
    _c += H[_k] // 8
RW = _r
OWN = _c
CG = OWN + 13
HALF = RW // 2
PK = -(-CG // 32)
CORNER = OWN // 32

f32 = jnp.float32
bf16 = jnp.bfloat16
VMEM = pl.BlockSpec(memory_space=pltpu.VMEM)
HBM = pl.BlockSpec(memory_space=pltpu.HBM)
ANY = pl.BlockSpec(memory_space=pl.ANY)
SMALL = pltpu.CompilerParams(vmem_limit_bytes=6 << 20)


def iota(shape, dim):
    return lax.broadcasted_iota(jnp.int32, shape, dim)


def col_group(n, g):
    return OWN + n if g == H[PLANES[n][0]] // 8 else COFF[n] + g


def row_pack_kernel(d1, d2, d3, d4, coarse, up, down, *scratch):
    sources = (d1, d2, d3, d4, coarse)
    tops, bots, sems = scratch[:5], scratch[5:10], scratch[10]
    copies = []
    for n, src in enumerate(sources):
        last = src.shape[-2] - 8
        for side, at, dst in ((0, 0, tops[n]), (1, last, bots[n])):
            rows = src.at[pl.ds(at, 8), :] if n == 4 else src.at[:, pl.ds(at, 8), :]
            copies.append(pltpu.make_async_copy(rows, dst, sems.at[2 * n + side]))
    for c in copies:
        c.start()
    for c in copies:
        c.wait()

    def line(refs):
        return jnp.concatenate([refs[k][p] if p < 3 else refs[4][...] for k, p in PLANES], axis=1)

    top, bot = line(tops), line(bots)
    low = iota((8, HALF), 0) < 4
    up[...] = jnp.where(low, top[:, :HALF], pltpu.roll(top[:, HALF:], 4, 0))
    down[...] = jnp.where(low, pltpu.roll(bot[:, :HALF], 4, 0), bot[:, HALF:])


def row_pack(coarse, details):
    out = jax.ShapeDtypeStruct((8, HALF), f32)
    edges = [pltpu.VMEM((3, 8, w), f32) for w in W] + [pltpu.VMEM((8, W[3]), f32)]
    return pl.pallas_call(
        row_pack_kernel,
        in_specs=[HBM] * 5,
        out_specs=[VMEM] * 2,
        out_shape=[out, out],
        scratch_shapes=edges + edges + [pltpu.SemaphoreType.DMA((10,))],
        compiler_params=SMALL,
        name="row_pack",
    )(*(pltpu.with_memory_space_constraint(x, pltpu.HBM) for x in (*details, coarse)))


def row_unpack(after, before):
    low = iota(after.shape, 0) < 4
    first = jnp.where(low, after, pltpu.roll(before, 4, 0))
    second = jnp.where(low, pltpu.roll(after, 4, 0), before)
    return first, second


def place(edges, lacc, racc):
    lane = iota((8, 128), 1)
    for q, e in edges:
        m, j = divmod(q, 32)
        nxt = (4 * j + 4) % 128
        e = e()
        if nxt:
            e = pltpu.roll(e, nxt, 1)
        lacc[m] = jnp.where((lane >= nxt) & (lane < nxt + 4), e, lacc[m])
        racc[m] = jnp.where((lane >= 4 * j) & (lane < 4 * j + 4), e, racc[m])


def col_pack_kernel(d1, d2, d3, d4, coarse, _, left_out, right_out):
    details = (d1, d2, d3, d4)
    lane = iota((8, 128), 1)

    def edge(n, g):
        k, p = PLANES[n]
        rows = slice(8 * g, 8 * g + 8)
        if p == 3:
            return coarse[rows, :]
        lo, hi = details[k][p, rows, :128], details[k][p, rows, W[k] - 128 :]
        return jnp.where(lane < 64, lo, hi)

    order = {}
    for n, (k, p) in enumerate(PLANES):
        for g in range(H[k] // 8):
            order[COFF[n] + g] = functools.partial(edge, n, g)
    lacc = {m: jnp.zeros((8, 128), f32) for m in range(PK)}
    racc = {m: jnp.zeros((8, 128), f32) for m in range(PK)}
    place([(q, order[q]) for j in range(32) for q in range(j, OWN, 32)], lacc, racc)
    for m in range(PK):
        left_out[8 * m : 8 * m + 8, :] = lacc[m]
        right_out[8 * m : 8 * m + 8, :] = racc[m]


def corner_kernel(left, right, after, before, _, across, within):
    odd = lax.axis_index("cols") % 2 == 1
    first, second = row_unpack(after[...], before[...])
    lane = iota((8, 128), 1)
    across[...] = jnp.where(odd, right[...], left[...])
    within[...] = jnp.where(odd, left[...], right[...])

    def piece(o):
        return first[:, o : o + 128] if o < HALF else second[:, o - HALF : o - HALF + 128]

    def edge(n):
        return jnp.where(lane < 64, piece(ROFF[n]), piece(ROFF[n] + W[PLANES[n][0]] - 128))

    rows = slice(8 * CORNER, 8 * CORNER + 8)
    lacc, racc = {CORNER: left[rows, :]}, {CORNER: right[rows, :]}
    place([(OWN + n, functools.partial(edge, n)) for n in range(13)], lacc, racc)
    across[rows, :] = jnp.where(odd, racc[CORNER], lacc[CORNER])
    within[rows, :] = jnp.where(odd, lacc[CORNER], racc[CORNER])


def col_pack(coarse, details, after_this):
    out = jax.ShapeDtypeStruct((8 * PK, 128), f32)
    return pl.pallas_call(
        col_pack_kernel,
        in_specs=[VMEM] * 5 + [HBM],
        out_specs=[VMEM] * 2,
        out_shape=[out, out],
        compiler_params=SMALL,
        name="col_pack",
    )(*details, coarse, after_this)


def corners(left, right, after, before, after_this):
    out = jax.ShapeDtypeStruct((8 * PK, 128), f32)
    return pl.pallas_call(
        corner_kernel,
        in_specs=[VMEM] * 4 + [ANY],
        out_specs=[VMEM] * 2,
        out_shape=[out, out],
        compiler_params=SMALL,
        name="corners",
    )(left, right, after, before, after_this)


def vertical(load_s, load_r, groups, store_s, store_r):
    sub = iota((8, 128), 0)
    first, last = sub == 0, sub == 7

    def cached(f):
        memo = {}

        def get(g):
            g = g % groups
            if g not in memo:
                memo[g] = f(g)
            return memo[g]

        return get

    def prev_of(x):
        turned = cached(lambda g: pltpu.roll(x(g), 1, 0))
        return lambda g: jnp.where(first, turned(g - 1), turned(g))

    def next_of(x):
        turned = cached(lambda g: pltpu.roll(x(g), 7, 0))
        return lambda g: jnp.where(last, turned(g + 1), turned(g))

    s, r = cached(load_s), cached(load_r)
    rp = prev_of(r)
    s1 = cached(lambda g: s(g) - lift_delta * (r(g) + rp(g)))
    s1n = next_of(s1)
    r1 = cached(lambda g: r(g) - lift_gamma * (s1(g) + s1n(g)))
    r1p = prev_of(r1)
    s2 = cached(lambda g: s1(g) - lift_beta * (r1(g) + r1p(g)))
    s2n = next_of(s2)
    r2 = cached(lambda g: r1(g) - lift_alpha * (s2(g) + s2n(g)))
    for g in range(groups):
        store_s(g, s2(g))
        store_r(g, r2(g))


def lanes_of(b):
    return pl.ds(128 * b if isinstance(b, int) else pl.multiple_of(b * 128, 128), 128)


def interleaved_store(ref, odd, skip):
    def put(g, x):
        if g != skip:
            ref[pl.ds(16 * g + odd, 8, 2), :] = x

    return put


def high_columns(k, load, ref):
    groups = H[k] // 8 + 1
    skip = groups - 1 if k == 0 else -1
    vertical(
        lambda g: load(0, g),
        lambda g: load(2, g) * (1.0 / SQ),
        groups,
        interleaved_store(ref, 0, skip),
        interleaved_store(ref, 1, skip),
    )


def loop(n, f):
    if n == 1:
        f(0)
    else:
        lax.fori_loop(0, n, lambda i, c: (f(i), c)[1], 0)


def early_kernel(d1, _, v1):
    groups = H[0] // 8

    def columns(b):
        vertical(
            lambda g: d1[0, 8 * g : 8 * g + 8, lanes_of(b)],
            lambda g: d1[2, 8 * g : 8 * g + 8, lanes_of(b)] * (1.0 / SQ),
            groups,
            interleaved_store(v1.at[b], 0, -1),
            interleaved_store(v1.at[b], 1, -1),
        )

    loop(W[0] // 128, columns)


def early_columns(d1, after_this):
    return pl.pallas_call(
        early_kernel,
        in_specs=[VMEM, ANY],
        out_specs=VMEM,
        out_shape=jax.ShapeDtypeStruct((W[0] // 128, 2 * H[0], 128), f32),
        compiler_params=SMALL,
        name="early_columns",
    )(d1, after_this)


def detail_kernel(d1, d2, d3, d4, after, before, early, _, v1, v2, v3, v4, xr, perm):
    row = iota((512, 256), 0) % 256
    col = iota((512, 256), 1)
    target = jnp.where(row < 128, 2 * row, 2 * row - 255)
    perm[...] = jnp.where(col == target, 1.0, 0.0).astype(bf16)
    details, vs = (d1, d2, d3, d4), (v1, v2, v3, v4)
    first, second = row_unpack(after[...], before[...])
    xr[:, :HALF] = first
    xr[:, HALF:] = second
    for k in (3, 2, 1):
        def columns(b, k=k):
            def load(p, g):
                if g == H[k] // 8:
                    o = ROFF[3 * k + p]
                    if isinstance(b, int):
                        return xr[:, o + 128 * b : o + 128 * b + 128]
                    return xr[:, pl.ds(pl.multiple_of(o + b * 128, 128), 128)]
                return details[k][p, 8 * g : 8 * g + 8, lanes_of(b)]

            high_columns(k, load, vs[k].at[b])

        loop(W[k] // 128, columns)

    last = H[0] // 8 - 1
    around = (last - 1, last, last + 1, 0, 1)

    def load(p, b, i):
        g = around[i]
        if g > last:
            return xr[:, ROFF[p] + 128 * b : ROFF[p] + 128 * b + 128]
        return d1[p, 8 * g : 8 * g + 8, 128 * b : 128 * b + 128]

    def put(b, odd):
        def store(i, x):
            if i in (1, 3):
                v1[b, pl.ds(16 * around[i] + odd, 8, 2), :] = x

        return store

    for b in range(W[0] // 128):
        vertical(
            functools.partial(load, 0, b),
            lambda i, b=b: load(2, b, i) * (1.0 / SQ),
            5,
            put(b, 0),
            put(b, 1),
        )


def detail_columns(details, after, before, early, after_this):
    outs = [jax.ShapeDtypeStruct(early.shape, f32)]
    outs += [jax.ShapeDtypeStruct((W[k] // 128, 2 * H[k] + 16, 128), f32) for k in (1, 2, 3)]
    outs.append(jax.ShapeDtypeStruct((8, RW), f32))
    outs.append(jax.ShapeDtypeStruct((512, 256), bf16))
    return pl.pallas_call(
        detail_kernel,
        in_specs=[VMEM] * 7 + [ANY],
        out_specs=[VMEM] * 6,
        out_shape=outs,
        input_output_aliases={6: 0},
        compiler_params=SMALL,
        name="detail_columns",
    )(*details, after, before, early, after_this)


def interleave(s, r, blocks, perm, parts=2):
    rows = s.shape[0]
    x = jnp.concatenate(
        [
            jnp.concatenate([s[:, 128 * b : 128 * b + 128], r[:, 128 * b : 128 * b + 128]], axis=1)
            for b in range(blocks)
        ],
        axis=0,
    )
    hi = x.astype(bf16)
    lo = (x - hi.astype(f32)).astype(bf16)
    x = jnp.concatenate([hi, lo], axis=1)
    step = blocks * rows // parts // 16 * 16
    cuts = [*range(0, step * parts, step), blocks * rows]
    y = [
        jnp.dot(x[i:j, :], perm[...], preferred_element_type=f32) for i, j in zip(cuts[:-1], cuts[1:])
    ]
    y = jnp.concatenate(y, axis=0)
    return [y[rows * b : rows * b + rows, :] for b in range(blocks)]


CHUNK = (128, 88, 136, 144)
SLOTS = 4


def main_kernel(
    coarse, d4, d3, d2, d1, v1, v2, v3, v4, xr, perm, across, within, out,
    comb, u, vx, l3, l2, l1, s1, r1, s2, stage, sems,
):
    details, vs = (d1, d2, d3, d4), (v1, v2, v3, v4)
    lows = (l1, l2, l3)
    lane = iota((8, 128), 1)

    even = (iota((8 * PK, 128), 1) % 8) < 4
    odd = lax.axis_index("cols") % 2 == 1
    aft = jnp.where(odd, across[...], within[...])
    bef = jnp.where(odd, within[...], across[...])
    comb[0] = jnp.where(even, bef, aft)
    comb[1] = jnp.where(even, aft, bef)
    keep = (lane < 4) | (lane >= 124)

    def halo_column(q):
        m, j = divmod(q, 32)
        t = comb[j % 2, 8 * m : 8 * m + 8, :]
        shift = (124 - 4 * j) % 128
        if shift:
            t = pltpu.roll(t, shift, 1)
        return jnp.where(keep, t, 0.0)

    for k in (3, 2, 1, 0):
        h, w = H[k], W[k]
        groups, blocks = h // 8 + 1, w // 128
        skip = groups - 1 if k == 0 else -1

        def load(p, g, b, k=k, groups=groups, blocks=blocks):
            n = 3 * k + p if p < 3 else 12
            rows = slice(8 * g, 8 * g + 8)
            if p == 3 and k < 3:
                return lows[k][rows, lanes_of(b)]
            if isinstance(b, int) and b == blocks:
                return halo_column(col_group(n, g))
            if g == groups - 1:
                if isinstance(b, int):
                    return xr[:, ROFF[n] + 128 * b : ROFF[n] + 128 * b + 128]
                return xr[:, pl.ds(pl.multiple_of(ROFF[n] + b * 128, 128), 128)]
            if p == 3:
                return coarse[rows, lanes_of(b)]
            return details[k][p, rows, lanes_of(b)]

        def columns(b, load=load, groups=groups, skip=skip):
            vertical(
                lambda g: load(3, g, b) * SQ,
                lambda g: load(1, g, b),
                groups,
                interleaved_store(u.at[b], 0, skip),
                interleaved_store(u.at[b], 1, skip),
            )

        if blocks < 3:
            for b in range(blocks):
                columns(b)
        else:
            loop(blocks, columns)
        columns(blocks)
        high_columns(k, lambda p, g, load=load, blocks=blocks: load(p, g, blocks), vx)

        rows = CHUNK[k]
        count = 2 * h // rows if k == 0 else 16 * groups // rows
        width = w + 128
        kept = blocks + (k > 0)

        def at_rows(i, rows=rows):
            return pl.ds(i * rows if isinstance(i, int) else pl.multiple_of(i * rows, 8), rows)

        def slot(i):
            return i & 3

        def u_rows(i, blocks=blocks):
            return jnp.concatenate([u[b, at_rows(i), :] for b in range(blocks + 1)], axis=1)

        def v_rows(i, blocks=blocks, k=k):
            return jnp.concatenate(
                [vs[k][b, at_rows(i), :] for b in range(blocks)] + [vx[at_rows(i), :]], axis=1
            )

        def held(ref, i, rows=rows, width=width):
            return ref.at[slot(i), pl.ds(0, rows), pl.ds(0, width)]

        def step1(i, width=width):
            r = v_rows(i)
            held(s1, i)[...] = u_rows(i) - lift_delta * (r + pltpu.roll(r, 1, 1))

        def step2(i, width=width):
            x = held(s1, i)[...]
            held(r1, i)[...] = v_rows(i) - lift_gamma * (x + pltpu.roll(x, width - 1, 1))

        def step3(i):
            x = held(r1, i)[...]
            held(s2, i)[...] = held(s1, i)[...] - lift_beta * (x + pltpu.roll(x, 1, 1))

        def step4(i, k=k, rows=rows, width=width, blocks=blocks, kept=kept):
            x = held(s2, i)[...]
            y = held(r1, i)[...] - lift_alpha * (x + pltpu.roll(x, width - 1, 1))
            parts = interleave(x, y, kept, perm)
            if k == 0:
                for b in range(blocks):
                    stage[i & (SLOTS - 1), :, 256 * b : 256 * b + 256] = parts[b]
                return
            low = lows[k - 1]
            for b in range(blocks):
                low[at_rows(i), 256 * b : 256 * b + 256] = parts[b]
            left, right = parts[blocks][:, :128], parts[blocks][:, 128:]
            low[at_rows(i), 256 * blocks : 256 * blocks + 128] = jnp.where(
                iota((rows, 128), 1) < 64, left, right
            )

        steps = (step1, step2, step3, step4)

        def turn(i, k=k, steps=steps, count=count, send=True):
            def active(j):
                return not isinstance(i, int) or 0 <= i - j < count

            if k == 0 and active(3) and send:
                if isinstance(i, int):
                    copy_out(i - 3 - SLOTS, wait=True)
                else:
                    pl.when(i - 3 >= SLOTS)(lambda: copy_out(i - 3 - SLOTS, wait=True))
            for j in reversed(range(4)):
                if active(j):
                    steps[j](i - j)
            if k == 0 and active(3) and send:
                copy_out(i - 3)

        def copy_out(i, wait=False, rows=rows):
            c = i & (SLOTS - 1)
            c = pltpu.make_async_copy(stage.at[c], out.at[at_rows(i), :], sems.at[c])
            if wait:
                c.wait()
            else:
                c.start()

        first, last = (3, count) if count > 6 else (0, 0)
        for i in range(first):
            turn(i)
        if last > first:
            lax.fori_loop(first, last, lambda i, c: (turn(i), c)[1], 0)
        if k:
            for i in range(last, count + 3):
                turn(i)
        else:
            turn(count)
            copy_out(count - 2 - SLOTS, wait=True)
            copy_out(count - 1 - SLOTS, wait=True)
            turn(count + 1, send=False)
            turn(count + 2, send=False)
            copy_out(count - 2)
            copy_out(count - 1)

        if k:
            low = lows[k - 1]
            top = low[2 * h : 2 * h + 8, :]
            bottom = low[2 * h + 8 : 2 * h + 16, :]
            low[2 * h : 2 * h + 8, :] = jnp.where(iota(top.shape, 0) < 4, top, bottom)
        else:
            for i in range(count - SLOTS, count):
                copy_out(i, wait=True)


def main(coarse, d4, d3, d2, d1, *rest):
    return pl.pallas_call(
        main_kernel,
        in_specs=[VMEM] * 13,
        out_specs=HBM,
        out_shape=jax.ShapeDtypeStruct((1024, 2048), f32),
        scratch_shapes=[
            pltpu.VMEM((2, 8 * PK, 128), f32),
            pltpu.VMEM((9, 1040, 128), f32),
            pltpu.VMEM((1040, 128), f32),
            pltpu.VMEM((144, 384), f32),
            pltpu.VMEM((272, 640), f32),
            pltpu.VMEM((528, 1152), f32),
            pltpu.VMEM((4, 176, 1152), f32),
            pltpu.VMEM((4, 176, 1152), f32),
            pltpu.VMEM((4, 176, 1152), f32),
            pltpu.VMEM((SLOTS, CHUNK[0], 2048), f32),
            pltpu.SemaphoreType.DMA((SLOTS,)),
        ],
        compiler_params=pltpu.CompilerParams(vmem_limit_bytes=32 << 20),
        name="synthesis",
    )(coarse, d4, d3, d2, d1, *rest)


def per_device(coarse, detail4, detail3, detail2, detail1):
    details = (detail1, detail2, detail3, detail4)

    n = lax.axis_size("rows")
    up, down = row_pack(coarse, details)
    rbefore = lax.ppermute(down, "rows", [(i, (i + 1) % n) for i in range(n)])
    rafter = lax.ppermute(up, "rows", [((i + 1) % n, i) for i in range(n)])
    packed = col_pack(coarse, details, up)
    early = early_columns(detail1, packed[0])
    sent = corners(*packed, rafter, rbefore, early)
    across = exchange(sent[0], 1)
    within = exchange(sent[1], 0)
    highs = detail_columns(details, rafter, rbefore, early, sent[1])
    return main(coarse, detail4, detail3, detail2, detail1, *highs, across, within)


def exchange(x, first):
    n = lax.axis_size("cols")
    pairs = [((first + i) % n, (first + i + 1) % n) for i in range(0, n, 2)]
    return lax.ppermute(x, "cols", pairs + [(j, i) for i, j in pairs])


def solution(mesh):
    return jax.shard_map(
        per_device,
        mesh=mesh,
        in_specs=(
            P("rows", "cols"),
            P(None, "rows", "cols"),
            P(None, "rows", "cols"),
            P(None, "rows", "cols"),
            P(None, "rows", "cols"),
        ),
        out_specs=P("rows", "cols"),
        check_vma=False,
    )
```

```python
import functools

import jax
import jax.numpy as jnp
from jax import lax
from jax.experimental import pallas as pl
from jax.experimental.pallas import tpu as pltpu
from jax.sharding import PartitionSpec as P

lift_alpha = -1.586134342059924
lift_beta = -0.052980118572961
lift_gamma = 0.882911075530934
lift_delta = 0.443506852043971
lift_scale = 1.149604398860241
SQ = lift_scale * lift_scale

H = (512, 256, 128, 64)
W = (1024, 512, 256, 128)
PLANES = tuple((k, p) for k in range(4) for p in range(3)) + ((3, 3),)
ROFF = []
COFF = []
_r = _c = 0
for _k, _p in PLANES:
    ROFF.append(_r)
    COFF.append(_c)
    _r += W[_k]
    _c += H[_k] // 8
RW = _r
OWN = _c
CG = OWN + 13
HALF = RW // 2
PK = -(-CG // 32)
CORNER = OWN // 32

f32 = jnp.float32
bf16 = jnp.bfloat16
VMEM = pl.BlockSpec(memory_space=pltpu.VMEM)
HBM = pl.BlockSpec(memory_space=pltpu.HBM)
ANY = pl.BlockSpec(memory_space=pl.ANY)
SMALL = pltpu.CompilerParams(vmem_limit_bytes=6 << 20)


def iota(shape, dim):
    return lax.broadcasted_iota(jnp.int32, shape, dim)


def col_group(n, g):
    return OWN + n if g == H[PLANES[n][0]] // 8 else COFF[n] + g


def row_pack_kernel(d1, d2, d3, d4, coarse, up, down, *scratch):
    sources = (d1, d2, d3, d4, coarse)
    tops, bots, sems = scratch[:5], scratch[5:10], scratch[10]
    copies = []
    for n, src in enumerate(sources):
        last = src.shape[-2] - 8
        for side, at, dst in ((0, 0, tops[n]), (1, last, bots[n])):
            rows = src.at[pl.ds(at, 8), :] if n == 4 else src.at[:, pl.ds(at, 8), :]
            copies.append(pltpu.make_async_copy(rows, dst, sems.at[2 * n + side]))
    for c in copies:
        c.start()
    for c in copies:
        c.wait()

    def line(refs):
        return jnp.concatenate([refs[k][p] if p < 3 else refs[4][...] for k, p in PLANES], axis=1)

    top, bot = line(tops), line(bots)
    low = iota((8, HALF), 0) < 4
    up[...] = jnp.where(low, top[:, :HALF], pltpu.roll(top[:, HALF:], 4, 0))
    down[...] = jnp.where(low, pltpu.roll(bot[:, :HALF], 4, 0), bot[:, HALF:])


def row_pack(coarse, details):
    out = jax.ShapeDtypeStruct((8, HALF), f32)
    edges = [pltpu.VMEM((3, 8, w), f32) for w in W] + [pltpu.VMEM((8, W[3]), f32)]
    return pl.pallas_call(
        row_pack_kernel,
        in_specs=[HBM] * 5,
        out_specs=[VMEM] * 2,
        out_shape=[out, out],
        scratch_shapes=edges + edges + [pltpu.SemaphoreType.DMA((10,))],
        compiler_params=SMALL,
        name="row_pack",
    )(*(pltpu.with_memory_space_constraint(x, pltpu.HBM) for x in (*details, coarse)))


def row_unpack(after, before):
    low = iota(after.shape, 0) < 4
    first = jnp.where(low, after, pltpu.roll(before, 4, 0))
    second = jnp.where(low, pltpu.roll(after, 4, 0), before)
    return first, second


def place(edges, lacc, racc):
    lane = iota((8, 128), 1)
    for q, e in edges:
        m, j = divmod(q, 32)
        nxt = (4 * j + 4) % 128
        e = e()
        if nxt:
            e = pltpu.roll(e, nxt, 1)
        lacc[m] = jnp.where((lane >= nxt) & (lane < nxt + 4), e, lacc[m])
        racc[m] = jnp.where((lane >= 4 * j) & (lane < 4 * j + 4), e, racc[m])


def col_pack_kernel(d1, d2, d3, d4, coarse, _, left_out, right_out):
    details = (d1, d2, d3, d4)
    lane = iota((8, 128), 1)

    def edge(n, g):
        k, p = PLANES[n]
        rows = slice(8 * g, 8 * g + 8)
        if p == 3:
            return coarse[rows, :]
        lo, hi = details[k][p, rows, :128], details[k][p, rows, W[k] - 128 :]
        return jnp.where(lane < 64, lo, hi)

    order = {}
    for n, (k, p) in enumerate(PLANES):
        for g in range(H[k] // 8):
            order[COFF[n] + g] = functools.partial(edge, n, g)
    lacc = {m: jnp.zeros((8, 128), f32) for m in range(PK)}
    racc = {m: jnp.zeros((8, 128), f32) for m in range(PK)}
    place([(q, order[q]) for j in range(32) for q in range(j, OWN, 32)], lacc, racc)
    for m in range(PK):
        left_out[8 * m : 8 * m + 8, :] = lacc[m]
        right_out[8 * m : 8 * m + 8, :] = racc[m]


def corner_kernel(left, right, after, before, _, across, within):
    odd = lax.axis_index("cols") % 2 == 1
    first, second = row_unpack(after[...], before[...])
    lane = iota((8, 128), 1)
    across[...] = jnp.where(odd, right[...], left[...])
    within[...] = jnp.where(odd, left[...], right[...])

    def piece(o):
        return first[:, o : o + 128] if o < HALF else second[:, o - HALF : o - HALF + 128]

    def edge(n):
        return jnp.where(lane < 64, piece(ROFF[n]), piece(ROFF[n] + W[PLANES[n][0]] - 128))

    rows = slice(8 * CORNER, 8 * CORNER + 8)
    lacc, racc = {CORNER: left[rows, :]}, {CORNER: right[rows, :]}
    place([(OWN + n, functools.partial(edge, n)) for n in range(13)], lacc, racc)
    across[rows, :] = jnp.where(odd, racc[CORNER], lacc[CORNER])
    within[rows, :] = jnp.where(odd, lacc[CORNER], racc[CORNER])


def col_pack(coarse, details, after_this):
    out = jax.ShapeDtypeStruct((8 * PK, 128), f32)
    return pl.pallas_call(
        col_pack_kernel,
        in_specs=[VMEM] * 5 + [HBM],
        out_specs=[VMEM] * 2,
        out_shape=[out, out],
        compiler_params=SMALL,
        name="col_pack",
    )(*details, coarse, after_this)


def corners(left, right, after, before, after_this):
    out = jax.ShapeDtypeStruct((8 * PK, 128), f32)
    return pl.pallas_call(
        corner_kernel,
        in_specs=[VMEM] * 4 + [ANY],
        out_specs=[VMEM] * 2,
        out_shape=[out, out],
        compiler_params=SMALL,
        name="corners",
    )(left, right, after, before, after_this)


def vertical(load_s, load_r, groups, store_s, store_r):
    sub = iota((8, 128), 0)
    first, last = sub == 0, sub == 7

    def cached(f):
        memo = {}

        def get(g):
            g = g % groups
            if g not in memo:
                memo[g] = f(g)
            return memo[g]

        return get

    def prev_of(x):
        turned = cached(lambda g: pltpu.roll(x(g), 1, 0))
        return lambda g: jnp.where(first, turned(g - 1), turned(g))

    def next_of(x):
        turned = cached(lambda g: pltpu.roll(x(g), 7, 0))
        return lambda g: jnp.where(last, turned(g + 1), turned(g))

    s, r = cached(load_s), cached(load_r)
    rp = prev_of(r)
    s1 = cached(lambda g: s(g) - lift_delta * (r(g) + rp(g)))
    s1n = next_of(s1)
    r1 = cached(lambda g: r(g) - lift_gamma * (s1(g) + s1n(g)))
    r1p = prev_of(r1)
    s2 = cached(lambda g: s1(g) - lift_beta * (r1(g) + r1p(g)))
    s2n = next_of(s2)
    r2 = cached(lambda g: r1(g) - lift_alpha * (s2(g) + s2n(g)))
    for g in range(groups):
        store_s(g, s2(g))
        store_r(g, r2(g))


def lanes_of(b):
    return pl.ds(128 * b if isinstance(b, int) else pl.multiple_of(b * 128, 128), 128)


def interleaved_store(ref, odd, skip):
    def put(g, x):
        if g != skip:
            ref[pl.ds(16 * g + odd, 8, 2), :] = x

    return put


def high_columns(k, load, ref):
    groups = H[k] // 8 + 1
    skip = groups - 1 if k == 0 else -1
    vertical(
        lambda g: load(0, g),
        lambda g: load(2, g) * (1.0 / SQ),
        groups,
        interleaved_store(ref, 0, skip),
        interleaved_store(ref, 1, skip),
    )


def loop(n, f):
    if n == 1:
        f(0)
    else:
        lax.fori_loop(0, n, lambda i, c: (f(i), c)[1], 0)


def early_kernel(d1, _, v1):
    groups = H[0] // 8

    def columns(b):
        vertical(
            lambda g: d1[0, 8 * g : 8 * g + 8, lanes_of(b)],
            lambda g: d1[2, 8 * g : 8 * g + 8, lanes_of(b)] * (1.0 / SQ),
            groups,
            interleaved_store(v1.at[b], 0, -1),
            interleaved_store(v1.at[b], 1, -1),
        )

    loop(W[0] // 128, columns)


def early_columns(d1, after_this):
    return pl.pallas_call(
        early_kernel,
        in_specs=[VMEM, ANY],
        out_specs=VMEM,
        out_shape=jax.ShapeDtypeStruct((W[0] // 128, 2 * H[0], 128), f32),
        compiler_params=SMALL,
        name="early_columns",
    )(d1, after_this)


def detail_kernel(d1, d2, d3, d4, after, before, early, _, v1, v2, v3, v4, xr, perm):
    row = iota((512, 256), 0) % 256
    col = iota((512, 256), 1)
    target = jnp.where(row < 128, 2 * row, 2 * row - 255)
    perm[...] = jnp.where(col == target, 1.0, 0.0).astype(bf16)
    details, vs = (d1, d2, d3, d4), (v1, v2, v3, v4)
    first, second = row_unpack(after[...], before[...])
    xr[:, :HALF] = first
    xr[:, HALF:] = second
    for k in (3, 2, 1):
        def columns(b, k=k):
            def load(p, g):
                if g == H[k] // 8:
                    o = ROFF[3 * k + p]
                    if isinstance(b, int):
                        return xr[:, o + 128 * b : o + 128 * b + 128]
                    return xr[:, pl.ds(pl.multiple_of(o + b * 128, 128), 128)]
                return details[k][p, 8 * g : 8 * g + 8, lanes_of(b)]

            high_columns(k, load, vs[k].at[b])

        loop(W[k] // 128, columns)

    last = H[0] // 8 - 1
    around = (last - 1, last, last + 1, 0, 1)

    def load(p, b, i):
        g = around[i]
        if g > last:
            return xr[:, ROFF[p] + 128 * b : ROFF[p] + 128 * b + 128]
        return d1[p, 8 * g : 8 * g + 8, 128 * b : 128 * b + 128]

    def put(b, odd):
        def store(i, x):
            if i in (1, 3):
                v1[b, pl.ds(16 * around[i] + odd, 8, 2), :] = x

        return store

    for b in range(W[0] // 128):
        vertical(
            functools.partial(load, 0, b),
            lambda i, b=b: load(2, b, i) * (1.0 / SQ),
            5,
            put(b, 0),
            put(b, 1),
        )


def detail_columns(details, after, before, early, after_this):
    outs = [jax.ShapeDtypeStruct(early.shape, f32)]
    outs += [jax.ShapeDtypeStruct((W[k] // 128, 2 * H[k] + 16, 128), f32) for k in (1, 2, 3)]
    outs.append(jax.ShapeDtypeStruct((8, RW), f32))
    outs.append(jax.ShapeDtypeStruct((512, 256), bf16))
    return pl.pallas_call(
        detail_kernel,
        in_specs=[VMEM] * 7 + [ANY],
        out_specs=[VMEM] * 6,
        out_shape=outs,
        input_output_aliases={6: 0},
        compiler_params=SMALL,
        name="detail_columns",
    )(*details, after, before, early, after_this)


def interleave(s, r, blocks, perm, parts=2):
    rows = s.shape[0]
    x = jnp.concatenate(
        [
            jnp.concatenate([s[:, 128 * b : 128 * b + 128], r[:, 128 * b : 128 * b + 128]], axis=1)
            for b in range(blocks)
        ],
        axis=0,
    )
    hi = x.astype(bf16)
    lo = (x - hi.astype(f32)).astype(bf16)
    x = jnp.concatenate([hi, lo], axis=1)
    step = blocks * rows // parts // 16 * 16
    cuts = [*range(0, step * parts, step), blocks * rows]
    y = [
        jnp.dot(x[i:j, :], perm[...], preferred_element_type=f32) for i, j in zip(cuts[:-1], cuts[1:])
    ]
    y = jnp.concatenate(y, axis=0)
    return [y[rows * b : rows * b + rows, :] for b in range(blocks)]


CHUNK = (128, 176, 136, 144)
SLOTS = 4


def main_kernel(
    coarse, d4, d3, d2, d1, v1, v2, v3, v4, xr, perm, across, within, out,
    comb, u, vx, l3, l2, l1, s1, r1, s2, stage, sems,
):
    details, vs = (d1, d2, d3, d4), (v1, v2, v3, v4)
    lows = (l1, l2, l3)
    lane = iota((8, 128), 1)

    even = (iota((8 * PK, 128), 1) % 8) < 4
    odd = lax.axis_index("cols") % 2 == 1
    aft = jnp.where(odd, across[...], within[...])
    bef = jnp.where(odd, within[...], across[...])
    comb[0] = jnp.where(even, bef, aft)
    comb[1] = jnp.where(even, aft, bef)
    keep = (lane < 4) | (lane >= 124)

    def halo_column(q):
        m, j = divmod(q, 32)
        t = comb[j % 2, 8 * m : 8 * m + 8, :]
        shift = (124 - 4 * j) % 128
        if shift:
            t = pltpu.roll(t, shift, 1)
        return jnp.where(keep, t, 0.0)

    for k in (3, 2, 1, 0):
        h, w = H[k], W[k]
        groups, blocks = h // 8 + 1, w // 128
        skip = groups - 1 if k == 0 else -1

        def load(p, g, b, k=k, groups=groups, blocks=blocks):
            n = 3 * k + p if p < 3 else 12
            rows = slice(8 * g, 8 * g + 8)
            if p == 3 and k < 3:
                return lows[k][rows, lanes_of(b)]
            if isinstance(b, int) and b == blocks:
                return halo_column(col_group(n, g))
            if g == groups - 1:
                if isinstance(b, int):
                    return xr[:, ROFF[n] + 128 * b : ROFF[n] + 128 * b + 128]
                return xr[:, pl.ds(pl.multiple_of(ROFF[n] + b * 128, 128), 128)]
            if p == 3:
                return coarse[rows, lanes_of(b)]
            return details[k][p, rows, lanes_of(b)]

        def columns(b, load=load, groups=groups, skip=skip):
            vertical(
                lambda g: load(3, g, b) * SQ,
                lambda g: load(1, g, b),
                groups,
                interleaved_store(u.at[b], 0, skip),
                interleaved_store(u.at[b], 1, skip),
            )

        if blocks < 3:
            for b in range(blocks):
                columns(b)
        else:
            loop(blocks, columns)
        columns(blocks)
        high_columns(k, lambda p, g, load=load, blocks=blocks: load(p, g, blocks), vx)

        rows = CHUNK[k]
        count = 2 * h // rows if k == 0 else 16 * groups // rows
        width = w + 128
        kept = blocks + (k > 0)

        def at_rows(i, rows=rows):
            return pl.ds(i * rows if isinstance(i, int) else pl.multiple_of(i * rows, 8), rows)

        def slot(i):
            return i & 3

        def u_rows(i, blocks=blocks):
            return jnp.concatenate([u[b, at_rows(i), :] for b in range(blocks + 1)], axis=1)

        def v_rows(i, blocks=blocks, k=k):
            return jnp.concatenate(
                [vs[k][b, at_rows(i), :] for b in range(blocks)] + [vx[at_rows(i), :]], axis=1
            )

        def held(ref, i, rows=rows, width=width):
            return ref.at[slot(i), pl.ds(0, rows), pl.ds(0, width)]

        def step1(i, width=width):
            r = v_rows(i)
            held(s1, i)[...] = u_rows(i) - lift_delta * (r + pltpu.roll(r, 1, 1))

        def step2(i, width=width):
            x = held(s1, i)[...]
            held(r1, i)[...] = v_rows(i) - lift_gamma * (x + pltpu.roll(x, width - 1, 1))

        def step3(i):
            x = held(r1, i)[...]
            held(s2, i)[...] = held(s1, i)[...] - lift_beta * (x + pltpu.roll(x, 1, 1))

        def step4(i, k=k, rows=rows, width=width, blocks=blocks, kept=kept):
            x = held(s2, i)[...]
            y = held(r1, i)[...] - lift_alpha * (x + pltpu.roll(x, width - 1, 1))
            parts = interleave(x, y, kept, perm)
            if k == 0:
                for b in range(blocks):
                    stage[i & (SLOTS - 1), :, 256 * b : 256 * b + 256] = parts[b]
                return
            low = lows[k - 1]
            for b in range(blocks):
                low[at_rows(i), 256 * b : 256 * b + 256] = parts[b]
            left, right = parts[blocks][:, :128], parts[blocks][:, 128:]
            low[at_rows(i), 256 * blocks : 256 * blocks + 128] = jnp.where(
                iota((rows, 128), 1) < 64, left, right
            )

        steps = (step1, step2, step3, step4)

        def turn(i, k=k, steps=steps, count=count, send=True):
            def active(j):
                return not isinstance(i, int) or 0 <= i - j < count

            if k == 0 and active(3) and send:
                if isinstance(i, int):
                    copy_out(i - 3 - SLOTS, wait=True)
                else:
                    pl.when(i - 3 >= SLOTS)(lambda: copy_out(i - 3 - SLOTS, wait=True))
            for j in reversed(range(4)):
                if active(j):
                    steps[j](i - j)
            if k == 0 and active(3) and send:
                copy_out(i - 3)

        def copy_out(i, wait=False, rows=rows):
            c = i & (SLOTS - 1)
            c = pltpu.make_async_copy(stage.at[c], out.at[at_rows(i), :], sems.at[c])
            if wait:
                c.wait()
            else:
                c.start()

        first, last = (3, count) if count > 6 else (0, 0)
        for i in range(first):
            turn(i)
        if last > first:
            lax.fori_loop(first, last, lambda i, c: (turn(i), c)[1], 0)
        if k:
            for i in range(last, count + 3):
                turn(i)
        else:
            turn(count)
            copy_out(count - 2 - SLOTS, wait=True)
            copy_out(count - 1 - SLOTS, wait=True)
            turn(count + 1, send=False)
            turn(count + 2, send=False)
            copy_out(count - 2)
            copy_out(count - 1)

        if k:
            low = lows[k - 1]
            top = low[2 * h : 2 * h + 8, :]
            bottom = low[2 * h + 8 : 2 * h + 16, :]
            low[2 * h : 2 * h + 8, :] = jnp.where(iota(top.shape, 0) < 4, top, bottom)
        else:
            for i in range(count - SLOTS, count):
                copy_out(i, wait=True)


def main(coarse, d4, d3, d2, d1, *rest):
    return pl.pallas_call(
        main_kernel,
        in_specs=[VMEM] * 13,
        out_specs=HBM,
        out_shape=jax.ShapeDtypeStruct((1024, 2048), f32),
        scratch_shapes=[
            pltpu.VMEM((2, 8 * PK, 128), f32),
            pltpu.VMEM((9, 1040, 128), f32),
            pltpu.VMEM((1040, 128), f32),
            pltpu.VMEM((144, 384), f32),
            pltpu.VMEM((272, 640), f32),
            pltpu.VMEM((528, 1152), f32),
            pltpu.VMEM((4, 176, 1152), f32),
            pltpu.VMEM((4, 176, 1152), f32),
            pltpu.VMEM((4, 176, 1152), f32),
            pltpu.VMEM((SLOTS, CHUNK[0], 2048), f32),
            pltpu.SemaphoreType.DMA((SLOTS,)),
        ],
        compiler_params=pltpu.CompilerParams(vmem_limit_bytes=32 << 20),
        name="synthesis",
    )(coarse, d4, d3, d2, d1, *rest)


def per_device(coarse, detail4, detail3, detail2, detail1):
    details = (detail1, detail2, detail3, detail4)

    n = lax.axis_size("rows")
    up, down = row_pack(coarse, details)
    rbefore = lax.ppermute(down, "rows", [(i, (i + 1) % n) for i in range(n)])
    rafter = lax.ppermute(up, "rows", [((i + 1) % n, i) for i in range(n)])
    packed = col_pack(coarse, details, up)
    early = early_columns(detail1, packed[0])
    sent = corners(*packed, rafter, rbefore, early)
    across = exchange(sent[0], 1)
    within = exchange(sent[1], 0)
    highs = detail_columns(details, rafter, rbefore, early, sent[1])
    return main(coarse, detail4, detail3, detail2, detail1, *highs, across, within)


def exchange(x, first):
    n = lax.axis_size("cols")
    pairs = [((first + i) % n, (first + i + 1) % n) for i in range(0, n, 2)]
    return lax.ppermute(x, "cols", pairs + [(j, i) for i, j in pairs])


def solution(mesh):
    return jax.shard_map(
        per_device,
        mesh=mesh,
        in_specs=(
            P("rows", "cols"),
            P(None, "rows", "cols"),
            P(None, "rows", "cols"),
            P(None, "rows", "cols"),
            P(None, "rows", "cols"),
        ),
        out_specs=P("rows", "cols"),
        check_vma=False,
    )
```
